32 devices in a mesh: elem: 8 (over z, y), chan: 4 (over x, core).
Axes of the slice: x: 2, y: 2, z: 4, core: 2. Of those that a mesh axis runs over, the one named last changes fastest.
Arguments:
- voltages: bfloat16 [2, 1024, 19584], P(None, ('elem', 'chan')), may hold values from -6 to 6
- delays: int32 [1024], P(('elem', 'chan')), may hold values from 0 to 127
- prototype: bfloat16 [16, 1024], replicated, may hold values from -1.5 to 1.5
- subband_map: int32 [16], replicated, may hold values from 0 to 1023, as said below
- beam_weights: bfloat16 [512, 2, 16, 1024], P('elem', None, 'chan'), may hold values from -0.25 to 0.25
Outputs:
- element_power: bfloat16 [1024, 1024], P(('elem', 'chan'))
- beam_voltages: float32 [2, 64, 512], P(None, 'chan', 'elem')
The draws below stay inside these ranges and needn't reach their ends.
Inputs may be any that keep to these rules, and one draw needn't show every extreme that they name: `subband_map`: distinct channel numbers.
All inputs are finite; a program needn't handle non-finite values.
Results may differ from the reference program's by a relative error of at most 0.007.
Values may be sent and summed in bfloat16 or wider, within the bound.
A program may use at most 128 MiB of HBM per device.

```python
import math
import jax
import jax.numpy as jnp
from jax import lax

CH = 1024
TAPS = 16
BEAMS = 512
E_DEV = 32
FRAMES = 4
MAXD = 128
ELEMS = 1024
SUB = 16
SAMP = 19584


def draw_subband_map(key, part):
    return jax.random.permutation(key, CH)[:SUB].astype(jnp.int32)


def plant(values, rng, smallest, top_value):
    extent = values.shape
    index_at = [jax.random.randint(jax.random.fold_in(rng, axis), (), 0, extent[axis]) for axis in range(len(extent))]
    values = values.at[tuple(index_at)].set(smallest)
    longest = extent.index(max(extent))
    index_at[longest] = (index_at[longest] + 1) % extent[longest]
    return values.at[tuple(index_at)].set(top_value)


def with_spikes(result, key, source, target, parts, factor):
    def block_of(position):
        return (jnp.arange(result.shape[position]) // (result.shape[position] // parts)).reshape((-1,) + (1,) * (result.ndim - 1 - position))

    near = jax.random.permutation(key, parts)[block_of(target)]
    other_side = (block_of(target) + parts // 2) % parts
    return jnp.where((block_of(source) == near) | (block_of(source) == other_side), factor * result, result)


def block_levels(key, extent, split, least, high):
    def one(axis_at, blocks):
        draws = jax.random.uniform(jax.random.fold_in(jax.random.fold_in(key, 6), axis_at), (blocks,), jnp.float32, least / len(split), high / len(split))
        return jnp.repeat(jnp.exp(draws), extent[axis_at] // blocks).reshape((-1,) + (1,) * (len(extent) - axis_at - 1))

    gain = one(*split[0])
    for cut in split[1:]:
        gain = gain * one(*cut)
    return gain


def normal_values(stream_key, extent, scale, limit, shards=(), held_as=jnp.bfloat16):
    entries = scale * jax.random.normal(stream_key, extent, jnp.float32)
    if shards:
        entries = entries * block_levels(stream_key, extent, shards, -0.22, 0.18)
    return jnp.clip(entries, -limit, limit).astype(held_as)


def bell_draw_with(own_key, dims, spread, bound, split, heavy, kind=jnp.bfloat16):
    drawn = spread * jax.random.normal(own_key, dims, jnp.float32)
    if split:
        drawn = drawn * block_levels(own_key, dims, split, -0.22, 0.18)
    return jnp.clip(with_spikes(drawn, jax.random.fold_in(own_key, 3), *heavy), -bound, bound).astype(kind)


def setup_inputs(seed: int = 0) -> dict:
    seeds = jax.random.split(jax.random.key(seed), 6)
    voltages = normal_values(seeds[0], (2, ELEMS, SAMP), 1.0, 6.0, ((1, 32),))
    delays = plant(jax.random.randint(seeds[1], (ELEMS,), 0, MAXD), jax.random.fold_in(seeds[1], 1), 0, MAXD - 1).astype(jnp.int32)
    prototype = normal_values(seeds[2], (TAPS, CH), 0.25, 1.5)
    subband_map = draw_subband_map(jax.random.fold_in(seeds[5], 71), 0)
    beam_weights = bell_draw_with(seeds[4], (BEAMS, 2, SUB, ELEMS), ELEMS ** -0.5, 0.25, ((0, 8), (2, 4)), (3, 0, 8, 2.0))
    return {"voltages": voltages, "delays": delays, "prototype": prototype, "subband_map": subband_map, "beam_weights": beam_weights}


def filtered(voltages, delays, prototype):
    tap_count, chan_count = prototype.shape
    blocks = FRAMES + tap_count - 1
    window_len = blocks * chan_count

    def window(samples, offset):
        return lax.dynamic_slice_in_dim(samples, offset, window_len, 0)
    segments = jax.vmap(jax.vmap(window, in_axes=(0, 0)), in_axes=(0, None))(voltages, delays.astype(jnp.int32))
    segments = segments.reshape(voltages.shape[0], voltages.shape[1], blocks, chan_count)
    coeffs = prototype.astype(jnp.float32)
    running = jnp.zeros((voltages.shape[0], voltages.shape[1], FRAMES, chan_count), jnp.float32)
    for tap_index in range(tap_count):
        running = running + coeffs[tap_index] * segments[:, :, tap_index:tap_index + FRAMES, :].astype(jnp.float32)
    return running.astype(jnp.bfloat16)

def reference(voltages, delays, prototype, subband_map, beam_weights):
    groups = ELEMS // E_DEV

    def one_group(number):
        first_elem = number * E_DEV
        voltage_block = lax.dynamic_slice_in_dim(voltages, first_elem, E_DEV, 1)
        shifts = lax.dynamic_slice_in_dim(delays, first_elem, E_DEV, 0)
        filtered_wave = filtered(voltage_block, shifts, prototype)
        signal = filtered_wave[0].astype(jnp.float32) + 1j * filtered_wave[1].astype(jnp.float32)
        spectrum = jnp.fft.fft(signal, axis=-1) / math.sqrt(CH)
        spec_real = jnp.real(spectrum)
        spec_imag = jnp.imag(spectrum)
        power_block = lax.optimization_barrier(jnp.mean(spec_real * spec_real + spec_imag * spec_imag, axis=1)).astype(jnp.bfloat16)
        chosen = jnp.stack([spec_real[:, :, subband_map], spec_imag[:, :, subband_map]]).astype(jnp.bfloat16)
        return (power_block, chosen)
    power_all, chosen_groups = lax.map(one_group, jnp.arange(groups, dtype=jnp.int32))
    element_power = power_all.reshape(ELEMS, CH)
    chosen_all = jnp.transpose(chosen_groups, (1, 4, 3, 0, 2)).reshape(2, SUB, FRAMES, ELEMS)

    def one_subband(number):
        weight_slice = lax.dynamic_index_in_dim(beam_weights, number, 2, keepdims=False)
        spec_slice = lax.dynamic_index_in_dim(chosen_all, number, 1, keepdims=False)

        def contract(spectral, weighting):
            return jnp.dot(spectral, weighting.T, preferred_element_type=jnp.float32)
        out_real = contract(spec_slice[0], weight_slice[:, 0]) - contract(spec_slice[1], weight_slice[:, 1])
        out_imag = contract(spec_slice[1], weight_slice[:, 0]) + contract(spec_slice[0], weight_slice[:, 1])
        return jnp.stack([out_real, out_imag])
    stacked = lax.map(one_subband, jnp.arange(SUB, dtype=jnp.int32))
    beam_voltages = jnp.transpose(stacked, (1, 0, 2, 3)).reshape(2, SUB * FRAMES, BEAMS)
    return (element_power, beam_voltages)
```

```python
import functools
import math

import jax
import jax.numpy as jnp
import numpy as np
from jax import lax
from jax.experimental import pallas as pl
from jax.experimental.pallas import tpu as pltpu
from jax.sharding import PartitionSpec as P

FRAMES = 4
LANES = 128
ROWS = 8
RADIX = 8
LOGICAL = pl.DeviceIdType.LOGICAL
NT = (((1,), (1,)), ((), ()))
TN = (((0,), (0,)), ((), ()))


def cosine(turns, chan):
    y = jnp.abs((turns & (chan - 1)) - chan // 2) - chan // 4
    x = y.astype(jnp.float32) * (2.0 * math.pi / chan)
    s = x * x
    poly = 1.0 / 362880 - s * (1.0 / 39916800)
    poly = -1.0 / 5040 + s * poly
    poly = 1.0 / 120 + s * poly
    poly = -1.0 / 6 + s * poly
    return x + x * s * poly


def sine(turns, chan):
    return cosine(turns + 3 * (chan // 4), chan)


def eight_points(x):
    def add(a, b):
        return (a[0] + b[0], a[1] + b[1])

    def sub(a, b):
        return (a[0] - b[0], a[1] - b[1])

    def minus_i(a):
        return (a[1], -a[0])

    def four(v):
        a, b = add(v[0], v[2]), sub(v[0], v[2])
        c, d = add(v[1], v[3]), minus_i(sub(v[1], v[3]))
        return [add(a, c), add(b, d), sub(a, c), sub(b, d)]

    root = math.sqrt(0.5)
    even = four([add(x[a], x[a + 4]) for a in range(4)])
    d = [sub(x[a], x[a + 4]) for a in range(4)]
    d1 = ((d[1][0] + d[1][1]) * root, (d[1][1] - d[1][0]) * root)
    d3 = ((d[3][1] - d[3][0]) * root, (-d[3][0] - d[3][1]) * root)
    odd = four([d[0], d1, minus_i(d[2]), d3])
    out = []
    for e, o in zip(even, odd):
        out += [e, o]
    return out


def turn_plan(group, delay_ref):
    lane = lax.broadcasted_iota(jnp.int32, (ROWS, LANES), 1)
    sub = lax.broadcasted_iota(jnp.int32, (ROWS, LANES), 0)
    shift = jnp.zeros((ROWS, LANES), jnp.int32)
    for i in range(ROWS):
        shift = jnp.where(sub == i, delay_ref[group * ROWS + i], shift)
    return (lane - shift) & (LANES - 1), lane < shift


def turn_tap(t, slot, plan, base_ref, coef_ref):
    index, early = plan
    per = base_ref.shape[2] // LANES
    turned = [
        jnp.take_along_axis(
            base_ref[t, :, pl.ds(j * LANES, LANES)], index, axis=1, mode="promise_in_bounds"
        )
        for j in range(per)
    ]
    for j in range(per):
        coef_ref[slot, t, :, pl.ds(j * LANES, LANES)] = jnp.where(
            early, turned[(j - 1) % per], turned[j]
        )


def filter_column(group, part, chunk, j, slot, early, volt_ref, coef_ref, wave_ref):
    _, taps, _, chan = coef_ref.shape
    per = chan // LANES
    blocks = FRAMES + taps - 1
    held = [
        volt_ref[chunk, :, pl.ds((b * per + j) * LANES, LANES)].astype(jnp.float32)
        for b in range(blocks + (j == 0))
    ]
    if j == 0:
        held = [jnp.where(early, held[b + 1], held[b]) for b in range(blocks)]
    sums = [None] * FRAMES
    for t in range(taps):
        coef = coef_ref[slot, t, :, pl.ds(j * LANES, LANES)]
        for f in range(FRAMES):
            term = coef * held[f + t]
            sums[f] = term if t == 0 else sums[f] + term
    for f in range(0, FRAMES, 2):
        where = (group * FRAMES + f) * ROWS
        wave_ref[part, pl.ds(where, 2 * ROWS), pl.ds(j * LANES, LANES)] = jnp.concatenate(
            sums[f : f + 2], axis=0
        ).astype(jnp.bfloat16)


def main_kernel(
    nelem,
    nchan,
    gather,
    delay_hbm,
    map_hbm,
    volt_hbm,
    proto_hbm,
    weight_hbm,
    basis_hbm,
    power_ref,
    beam_ref,
    delay_ref,
    map_ref,
    volt_ref,
    proto_ref,
    raw_ref,
    basis_ref,
    base_ref,
    coef_ref,
    pick_ref,
    wave_ref,
    weight_ref,
    turned_ref,
    send_ref,
    recv_ref,
    local_sem,
    volt_sem,
    send_sem,
    recv_sem,
):
    parts, wave_rows, chan = wave_ref.shape
    chunks = volt_ref.shape[0]
    groups = chunks // parts
    elems = groups * ROWS
    taps = proto_ref.shape[0]
    per = chan // LANES
    count = nelem * nchan
    elem_at, chan_at = lax.axis_index("elem"), lax.axis_index("chan")
    me = elem_at * nchan + chan_at
    near_start = elem_at < nelem // 2
    barrier = pltpu.get_barrier_semaphore()

    def each_partner(act):
        def row(k, carry):
            first = jnp.where(near_start, nelem - 1 - k, k) * nchan
            for c in range(nchan):

                @pl.when(first + c != me)
                def _():
                    act(first + c, c)

            return carry

        if count <= 64:
            for k in range(nelem):
                row(k, 0)
        else:
            lax.fori_loop(0, nelem, row, 0)

    order = [(g, r) for g in [*range(1, groups), 0] for r in range(parts)]
    map_copy = pltpu.make_async_copy(map_hbm, map_ref, local_sem.at[0])
    proto_copy = pltpu.make_async_copy(proto_hbm, proto_ref, local_sem.at[1])
    delay_copy = pltpu.make_async_copy(delay_hbm, delay_ref, local_sem.at[2])
    basis_copy = pltpu.make_async_copy(basis_hbm, basis_ref, local_sem.at[3])
    weight_copy = pltpu.make_async_copy(weight_hbm, raw_ref, local_sem.at[4])
    ahead = volt_sem.shape[0]
    volt_copies = [
        pltpu.make_async_copy(
            volt_hbm.at[r, pl.ds(g * ROWS, ROWS)], volt_ref.at[k], volt_sem.at[k % ahead]
        )
        for k, (g, r) in enumerate(order)
    ]
    proto_copy.start()
    delay_copy.start()
    map_copy.start()
    for copy in volt_copies[:ahead]:
        copy.start()

    def greet(other, c):
        pl.semaphore_signal(barrier, inc=1, device_id=other, device_id_type=LOGICAL)

    each_partner(greet)

    proto_copy.wait()
    for t in range(taps):
        base_ref[t] = jnp.broadcast_to(
            proto_ref[pl.ds(t, 1), :].astype(jnp.float32), (ROWS, chan)
        )
    delay_copy.wait()
    plan = turn_plan(order[0][0], delay_ref)
    for t in range(taps):
        turn_tap(t, 0, plan, base_ref, coef_ref)

    map_copy.wait()
    subbands = map_ref.shape[0]
    block = subbands // nchan
    row = lax.broadcasted_iota(jnp.int32, (subbands, LANES), 0)
    lane = lax.broadcasted_iota(jnp.int32, (subbands, LANES), 1)
    wanted = jnp.zeros((subbands, LANES), jnp.int32)
    for s in range(subbands):
        wanted = jnp.where(row == s, map_ref[s], wanted)
    scale = chan**-0.5
    cos, sin = cosine(wanted * lane, chan) * scale, sine(wanted * lane, chan) * scale
    cos_step, sin_step = cosine(wanted * LANES, chan), sine(wanted * LANES, chan)
    for j in range(per):
        if j:
            cos, sin = cos * cos_step - sin * sin_step, sin * cos_step + cos * sin_step
        where = pl.ds(j * LANES, LANES)
        pick_ref[0, pl.ds(0, subbands), where] = cos.astype(jnp.bfloat16)
        pick_ref[0, pl.ds(subbands, subbands), where] = (-sin).astype(jnp.bfloat16)
        pick_ref[1, pl.ds(0, subbands), where] = sin.astype(jnp.bfloat16)
        pick_ref[1, pl.ds(subbands, subbands), where] = cos.astype(jnp.bfloat16)
    column = lax.broadcasted_iota(jnp.int32, (ROWS, LANES), 1)
    column = column // (FRAMES * ROWS) * ROWS + column % ROWS
    late = jnp.zeros((ROWS, LANES), jnp.int32)
    for e in range(elems):
        late = jnp.where(column == e, delay_ref[e], late)
    late = jnp.concatenate([late] * (subbands // ROWS), axis=0)
    cos_late, sin_late = cosine(wanted * late, chan), sine(wanted * late, chan)

    def arrive(k):
        volt_copies[k].wait()
        if k + ahead < chunks:
            volt_copies[k + ahead].start()
        elif k + ahead == chunks:
            basis_copy.start()
            weight_copy.start()

    span = FRAMES * ROWS
    inside = lane // span
    chosen = [None, None]
    for k, (g, r) in enumerate(order):
        arrive(k)
        slot = k // parts % 2
        if r == 0:
            early = plan[1]
            if k + parts < chunks:
                plan = turn_plan(order[k + parts][0], delay_ref)
        both = None
        for j in range(per):
            filter_column(g, r, k, j, slot, early, volt_ref, coef_ref, wave_ref)
            if k + parts < chunks:
                here = taps // parts
                for t in range(r * here + j * here // per, r * here + (j + 1) * here // per):
                    turn_tap(t, 1 - slot, plan, base_ref, coef_ref)
        if r == parts - 1:
            both = sum(
                lax.dot_general(
                    pick_ref[q],
                    wave_ref[q, pl.ds(g * span, span)],
                    NT,
                    preferred_element_type=jnp.float32,
                )
                for q in range(parts)
            )
            if span < LANES:
                both = jnp.concatenate(
                    [both, jnp.zeros((both.shape[0], LANES - span), jnp.float32)], axis=1
                )
            if g:
                both = pltpu.roll(both, g * span, 1)
            for i in range(2):
                piece = both[i * subbands : (i + 1) * subbands]
                chosen[i] = (
                    piece if chosen[i] is None else jnp.where(inside == g, piece, chosen[i])
                )
    real = chosen[0] * cos_late - chosen[1] * sin_late
    imag = chosen[1] * cos_late + chosen[0] * sin_late
    for c in range(nchan):
        part = slice(c * block, (c + 1) * block)
        send_ref[c] = jnp.concatenate([real[part], imag[part]], axis=0).astype(jnp.bfloat16)

    pl.semaphore_wait(barrier, count - 1)
    my_set = me // gather

    def send(other, c):
        pltpu.make_async_remote_copy(
            src_ref=send_ref.at[c],
            dst_ref=recv_ref.at[me],
            send_sem=send_sem,
            recv_sem=recv_sem.at[my_set],
            device_id=other,
            device_id_type=LOGICAL,
        ).start()

    each_partner(send)
    recv_ref[me] = send_ref[chan_at]

    lanes = chan // RADIX
    wave = [wave_ref[r] for r in range(2)]
    split_wave = [
        tuple(wave[r][:, a * lanes : (a + 1) * lanes].astype(jnp.float32) for r in range(2))
        for a in range(RADIX)
    ]
    classes = eight_points(split_wave)
    basis_copy.wait()
    powers = []
    for c in range(RADIX):
        mixed = jnp.concatenate(classes[c], axis=1).astype(jnp.bfloat16)
        spec = jnp.dot(mixed, basis_ref[c], preferred_element_type=jnp.float32)
        both = spec[:, :lanes] * spec[:, :lanes] + spec[:, lanes:] * spec[:, lanes:]
        totals = []
        for g in range(groups):
            tiles = [
                both[(g * FRAMES + f) * ROWS : (g * FRAMES + f + 1) * ROWS] for f in range(FRAMES)
            ]
            totals.append(sum(tiles[1:], tiles[0]))
        powers.append(jnp.concatenate(totals, axis=0) * (1.0 / FRAMES))
    wide = lanes // RADIX
    at = lax.broadcasted_iota(jnp.int32, (elems, lanes), 1)
    mixed = []
    for e in range(RADIX):
        piece = None
        for c in range(RADIX):
            shift = (wide * (c - e)) % lanes
            moved = pltpu.roll(powers[c], shift, 1) if shift else powers[c]
            piece = moved if piece is None else jnp.where(at // wide == c, moved, piece)
        mixed.append(piece)
    mixed = jnp.concatenate(mixed, axis=0).astype(jnp.bfloat16)
    down = lax.broadcasted_iota(jnp.int32, (lanes, lanes), 0)
    over = lax.broadcasted_iota(jnp.int32, (lanes, lanes), 1)
    back = (over == (down % wide) * RADIX + down // wide).astype(jnp.float32)
    final = jnp.dot(mixed, back.astype(jnp.bfloat16), preferred_element_type=jnp.float32)
    for e in range(RADIX):
        power_ref[:, e * lanes : (e + 1) * lanes] = final[e * elems : (e + 1) * elems].astype(
            jnp.bfloat16
        )

    beams = raw_ref.shape[0]
    weight_rows, total = weight_ref.shape
    wide_beams = turned_ref.shape[1] // block
    down = lax.broadcasted_iota(jnp.int32, (weight_rows, block * wide_beams), 0)
    over = lax.broadcasted_iota(jnp.int32, (weight_rows, block * wide_beams), 1)
    target = down % block * wide_beams + down // block % 2 * (wide_beams // 2)
    sort = (over == target + down // (2 * block)).astype(jnp.float32).astype(jnp.bfloat16)
    weight_copy.wait()
    step = min(8, beams)
    for i in range(0, beams, step):
        piece = raw_ref[i : i + step].reshape(step * 2 * block, raw_ref.shape[3])
        weight_ref[2 * block * i : 2 * block * (i + step)] = piece
    fan = LANES // elems

    def turn_weights(q, carry):
        depth = min(total, 8 * LANES)
        where = pl.multiple_of(q * depth, depth)
        turned = lax.dot_general(
            weight_ref[:, pl.ds(where, depth)], sort, TN, preferred_element_type=jnp.float32
        )
        for z in range(0, depth, LANES):
            tiles = [
                turned[z + (i * groups + g) * ROWS : z + (i * groups + g + 1) * ROWS]
                for g in range(groups)
                for i in range(fan)
            ]
            turned_ref[pl.ds(pl.multiple_of(where + z, LANES), LANES), :] = jnp.concatenate(
                tiles, axis=0
            ).astype(jnp.bfloat16)
        return carry

    if total <= 8 * LANES:
        turn_weights(0, 0)
    else:
        lax.fori_loop(0, total // (8 * LANES), turn_weights, 0)

    sets = count // gather
    place_at = lax.broadcasted_iota(jnp.int32, (2 * block, LANES), 1) // ROWS % fan
    low_row = lax.broadcasted_iota(jnp.int32, (2 * block, wide_beams), 0)

    def take(k, carry):
        which = jnp.where(near_start, k, sets - 1 - k)
        first = which * gather

        def arrived(n):
            some = recv_ref.at[pl.ds(0, n)]
            pltpu.make_async_copy(some, some, recv_sem.at[which]).wait()

        pl.when(which == my_set)(lambda: arrived(gather - 1))
        pl.when(which != my_set)(lambda: arrived(gather))
        pieces = [[] for _ in range(FRAMES)]
        for q in range(gather // fan):
            tiles = [recv_ref[first + q * fan + i].astype(jnp.float32) for i in range(fan)]
            for f in range(FRAMES):
                piece = None
                for i in range(fan):
                    shift = (ROWS * (i - f)) % LANES
                    moved = pltpu.roll(tiles[i], shift, 1) if shift else tiles[i]
                    piece = moved if piece is None else jnp.where(place_at == i, moved, piece)
                pieces[f].append(piece)
        picked = jnp.concatenate(
            [jnp.concatenate(p, axis=1) for p in pieces], axis=0
        ).astype(jnp.bfloat16)
        depth = gather * elems
        where = pl.multiple_of(which * depth, depth)
        product = jnp.dot(
            picked, turned_ref[pl.ds(where, depth), :], preferred_element_type=jnp.float32
        )
        out = []
        for f in range(FRAMES):
            tile = product[2 * block * f : 2 * block * (f + 1)]
            piece = tile[:, :wide_beams]
            for s in range(1, block):
                piece = jnp.where(
                    low_row % block == s, tile[:, s * wide_beams : (s + 1) * wide_beams], piece
                )
            out.append(piece if carry is None else carry[f] + piece)
        return tuple(out)

    if sets <= 8:
        sums = None
        for k in range(sets):
            sums = take(k, sums)
    else:
        zero = jnp.zeros((2 * block, wide_beams), jnp.float32)
        sums = lax.fori_loop(0, sets, take, (zero,) * FRAMES)
    for f in range(FRAMES):
        other = pltpu.roll(pltpu.roll(sums[f], wide_beams // 2, 1), block, 0)
        out = sums[f] + jnp.where(low_row < block, -other, other)
        for p in range(2):
            for s in range(block):
                at = p * block + s
                beam_ref[p, pl.ds(s * FRAMES + f, 1), :] = out[at : at + 1, :beams]

    sent = recv_ref.at[pl.ds(0, count - 1)]
    pltpu.make_async_copy(sent, sent, send_sem).wait()


def class_basis(chan):
    lanes = chan // RADIX
    b = np.arange(lanes)[:, None]
    d = np.arange(lanes)[None, :]
    out = []
    for c in range(RADIX):
        angle = 2.0 * np.pi / chan * (b * (c + RADIX * d) % chan)
        cos, sin = np.cos(angle) * chan**-0.5, np.sin(angle) * chan**-0.5
        out.append(np.block([[cos, -sin], [sin, cos]]))
    return jnp.asarray(np.stack(out), jnp.bfloat16)


def deliver_kernel(power_from, beam_from, power_to, beam_to, sems):
    copies = [
        pltpu.make_async_copy(power_from, power_to, sems.at[0]),
        pltpu.make_async_copy(beam_from, beam_to, sems.at[1]),
    ]
    for copy in copies:
        copy.start()
    for copy in copies:
        copy.wait()


def on_device(nelem, nchan, voltages, delays, prototype, subband_map, beam_weights):
    parts, elems, samples = voltages.shape
    taps, chan = prototype.shape
    beams, _, block, total = beam_weights.shape
    basis = class_basis(chan)
    count = nelem * nchan
    chunks = parts * elems // ROWS
    gather = 8
    wide_beams = max(LANES, 2 * beams)
    out_shape = [
        jax.ShapeDtypeStruct((elems, chan), jnp.bfloat16),
        jax.ShapeDtypeStruct((2, block * FRAMES, beams), jnp.float32),
    ]
    power, beam = pl.pallas_call(
        functools.partial(main_kernel, nelem, nchan, gather),
        in_specs=[pl.BlockSpec(memory_space=pltpu.HBM)] * 6,
        out_specs=[pl.BlockSpec(memory_space=pltpu.VMEM)] * 2,
        out_shape=[pltpu.VMEM(o.shape, o.dtype) for o in out_shape],
        scratch_shapes=[
            pltpu.SMEM(delays.shape, jnp.int32),
            pltpu.SMEM(subband_map.shape, jnp.int32),
            pltpu.VMEM((chunks, ROWS, samples), jnp.bfloat16),
            pltpu.VMEM((taps, chan), jnp.bfloat16),
            pltpu.VMEM(beam_weights.shape, jnp.bfloat16),
            pltpu.VMEM(basis.shape, jnp.bfloat16),
            pltpu.VMEM((taps, ROWS, chan), jnp.float32),
            pltpu.VMEM((2, taps, ROWS, chan), jnp.float32),
            pltpu.VMEM((2, 2 * subband_map.shape[0], chan), jnp.bfloat16),
            pltpu.VMEM((parts, FRAMES * elems, chan), jnp.bfloat16),
            pltpu.VMEM((beams * 2 * block, total), jnp.bfloat16),
            pltpu.VMEM((total, block * wide_beams), jnp.bfloat16),
            pltpu.VMEM((nchan, 2 * block, FRAMES * elems), jnp.bfloat16),
            pltpu.VMEM((count, 2 * block, FRAMES * elems), jnp.bfloat16),
            pltpu.SemaphoreType.DMA((5,)),
            pltpu.SemaphoreType.DMA((4,)),
            pltpu.SemaphoreType.DMA,
            pltpu.SemaphoreType.DMA((count // gather,)),
        ],
        compiler_params=pltpu.CompilerParams(
            collective_id=0, has_side_effects=True, vmem_limit_bytes=66_400_000
        ),
    )(delays, subband_map, voltages, prototype, beam_weights, basis)
    return pl.pallas_call(
        deliver_kernel,
        in_specs=[pl.BlockSpec(memory_space=pl.ANY)] * 2,
        out_specs=[pl.BlockSpec(memory_space=pl.ANY)] * 2,
        out_shape=out_shape,
        scratch_shapes=[pltpu.SemaphoreType.DMA((2,))],
        compiler_params=pltpu.CompilerParams(vmem_limit_bytes=2**20),
    )(power, beam)


def solution(mesh):
    return jax.shard_map(
        functools.partial(on_device, mesh.shape["elem"], mesh.shape["chan"]),
        mesh=mesh,
        in_specs=(
            P(None, ("elem", "chan"), None),
            P(("elem", "chan")),
            P(),
            P(),
            P("elem", None, "chan", None),
        ),
        out_specs=(P(("elem", "chan"), None), P(None, "chan", "elem")),
        check_vma=False,
    )
```

```python
import functools
import math

import jax
import jax.numpy as jnp
import numpy as np
from jax import lax
from jax.experimental import pallas as pl
from jax.experimental.pallas import tpu as pltpu
from jax.sharding import PartitionSpec as P

FRAMES = 4
LANES = 128
ROWS = 8
RADIX = 8
LOGICAL = pl.DeviceIdType.LOGICAL
NT = (((1,), (1,)), ((), ()))
TN = (((0,), (0,)), ((), ()))


def cosine(turns, chan):
    y = jnp.abs((turns & (chan - 1)) - chan // 2) - chan // 4
    x = y.astype(jnp.float32) * (2.0 * math.pi / chan)
    s = x * x
    poly = 1.0 / 362880 - s * (1.0 / 39916800)
    poly = -1.0 / 5040 + s * poly
    poly = 1.0 / 120 + s * poly
    poly = -1.0 / 6 + s * poly
    return x + x * s * poly


def sine(turns, chan):
    return cosine(turns + 3 * (chan // 4), chan)


def eight_points(x):
    def add(a, b):
        return (a[0] + b[0], a[1] + b[1])

    def sub(a, b):
        return (a[0] - b[0], a[1] - b[1])

    def minus_i(a):
        return (a[1], -a[0])

    def four(v):
        a, b = add(v[0], v[2]), sub(v[0], v[2])
        c, d = add(v[1], v[3]), minus_i(sub(v[1], v[3]))
        return [add(a, c), add(b, d), sub(a, c), sub(b, d)]

    root = math.sqrt(0.5)
    even = four([add(x[a], x[a + 4]) for a in range(4)])
    d = [sub(x[a], x[a + 4]) for a in range(4)]
    d1 = ((d[1][0] + d[1][1]) * root, (d[1][1] - d[1][0]) * root)
    d3 = ((d[3][1] - d[3][0]) * root, (-d[3][0] - d[3][1]) * root)
    odd = four([d[0], d1, minus_i(d[2]), d3])
    out = []
    for e, o in zip(even, odd):
        out += [e, o]
    return out


def turn_plan(group, delay_ref):
    lane = lax.broadcasted_iota(jnp.int32, (ROWS, LANES), 1)
    sub = lax.broadcasted_iota(jnp.int32, (ROWS, LANES), 0)
    shift = jnp.zeros((ROWS, LANES), jnp.int32)
    for i in range(ROWS):
        shift = jnp.where(sub == i, delay_ref[group * ROWS + i], shift)
    return (lane - shift) & (LANES - 1), lane < shift


def turn_pair(pair, slot, plan, proto_ref, turned_ref, coef_ref):
    index, early = plan
    taps, chan = proto_ref.shape
    per = chan // LANES
    first, last = 2 * pair, min(2 * pair + 2, per - 1)
    fresh = [*range(first, last), per - 1] if pair == 0 else range(first, last)
    for t in range(taps):
        for j in fresh:
            where = pl.ds(j * LANES, LANES)
            value = jnp.broadcast_to(proto_ref[pl.ds(t, 1), where], (ROWS, LANES))
            turned_ref[t, :, where] = jnp.take_along_axis(
                value, index, axis=1, mode="promise_in_bounds"
            )
        near = [
            turned_ref[t, :, pl.ds((first + i) % per * LANES, LANES)] for i in (-1, 0, 1)
        ]
        coef_ref[slot, t, :, pl.ds(first * LANES, 2 * LANES)] = jnp.concatenate(
            [jnp.where(early, near[0], near[1]), jnp.where(early, near[1], near[2])], axis=1
        ).astype(jnp.bfloat16)


def filter_pair(group, part, chunk, pair, slot, early, volt_ref, coef_ref, wave_ref):
    _, taps, _, chan = coef_ref.shape
    blocks = FRAMES + taps - 1
    wide = 2 * LANES

    def column(b, size):
        return volt_ref[chunk, :, pl.ds(b * chan + pair * wide, size)]

    held = [column(b, wide) for b in range(blocks)]
    if pair == 0:
        last = jnp.concatenate([column(blocks, LANES), held[-1][:, LANES:]], axis=1)
        held = [
            jnp.where(early, nxt, now) for now, nxt in zip(held, [*held[1:], last])
        ]
    stacks = [[] for _ in range(FRAMES)]
    for t in range(taps):
        coef = coef_ref[slot, t, :, pl.ds(pair * wide, wide)]
        for f in range(FRAMES):
            level, term = 0, coef * held[f + t]
            while stacks[f] and stacks[f][-1][0] == level:
                level, term = level + 1, stacks[f].pop()[1] + term
            stacks[f].append((level, term))
    for f in range(FRAMES):
        total = stacks[f].pop()[1]
        while stacks[f]:
            total = stacks[f].pop()[1] + total
        where = pl.ds((group * FRAMES + f) * ROWS, ROWS)
        wave_ref[part, where, pl.ds(pair * wide, wide)] = total


def main_kernel(
    nelem,
    nchan,
    gather,
    delay_hbm,
    map_hbm,
    volt_hbm,
    proto_hbm,
    weight_hbm,
    basis_hbm,
    power_ref,
    beam_ref,
    delay_ref,
    map_ref,
    volt_ref,
    proto_ref,
    raw_ref,
    basis_ref,
    wide_ref,
    spun_ref,
    coef_ref,
    pick_ref,
    wave_ref,
    weight_ref,
    turned_ref,
    send_ref,
    recv_ref,
    local_sem,
    volt_sem,
    send_sem,
    recv_sem,
):
    parts, wave_rows, chan = wave_ref.shape
    chunks = volt_ref.shape[0]
    groups = chunks // parts
    elems = groups * ROWS
    taps = proto_ref.shape[0]
    per = chan // LANES
    count = nelem * nchan
    elem_at, chan_at = lax.axis_index("elem"), lax.axis_index("chan")
    me = elem_at * nchan + chan_at
    near_start = elem_at < nelem // 2
    barrier = pltpu.get_barrier_semaphore()

    def each_partner(act):
        def row(k, carry):
            first = jnp.where(near_start, nelem - 1 - k, k) * nchan
            for c in range(nchan):

                @pl.when(first + c != me)
                def _():
                    act(first + c, c)

            return carry

        if count <= 64:
            for k in range(nelem):
                row(k, 0)
        else:
            lax.fori_loop(0, nelem, row, 0)

    order = [(g, r) for g in [*range(1, groups), 0] for r in range(parts)]
    map_copy = pltpu.make_async_copy(map_hbm, map_ref, local_sem.at[0])
    proto_copy = pltpu.make_async_copy(proto_hbm, proto_ref, local_sem.at[1])
    delay_copy = pltpu.make_async_copy(delay_hbm, delay_ref, local_sem.at[2])
    basis_copy = pltpu.make_async_copy(basis_hbm, basis_ref, local_sem.at[3])
    weight_copy = pltpu.make_async_copy(weight_hbm, raw_ref, local_sem.at[4])
    ahead = volt_sem.shape[0]
    volt_copies = [
        pltpu.make_async_copy(
            volt_hbm.at[r, pl.ds(g * ROWS, ROWS)], volt_ref.at[k], volt_sem.at[k % ahead]
        )
        for k, (g, r) in enumerate(order)
    ]
    proto_copy.start()
    delay_copy.start()
    map_copy.start()
    for copy in volt_copies[:ahead]:
        copy.start()

    def greet(other, c):
        pl.semaphore_signal(barrier, inc=1, device_id=other, device_id_type=LOGICAL)

    each_partner(greet)

    map_copy.wait()
    subbands = map_ref.shape[0]
    block = subbands // nchan
    row = lax.broadcasted_iota(jnp.int32, (subbands, LANES), 0)
    lane = lax.broadcasted_iota(jnp.int32, (subbands, LANES), 1)
    wanted = jnp.zeros((subbands, LANES), jnp.int32)
    for s in range(subbands):
        wanted = jnp.where(row == s, map_ref[s], wanted)
    scale = chan**-0.5
    cos, sin = cosine(wanted * lane, chan) * scale, sine(wanted * lane, chan) * scale
    cos_step, sin_step = cosine(wanted * LANES, chan), sine(wanted * LANES, chan)
    for j in range(per):
        if j:
            cos, sin = cos * cos_step - sin * sin_step, sin * cos_step + cos * sin_step
        where = pl.ds(j * LANES, LANES)
        pick_ref[0, pl.ds(0, subbands), where] = cos.astype(jnp.bfloat16)
        pick_ref[0, pl.ds(subbands, subbands), where] = (-sin).astype(jnp.bfloat16)
        pick_ref[1, pl.ds(0, subbands), where] = sin.astype(jnp.bfloat16)
        pick_ref[1, pl.ds(subbands, subbands), where] = cos.astype(jnp.bfloat16)
    delay_copy.wait()
    column = lax.broadcasted_iota(jnp.int32, (ROWS, LANES), 1)
    column = column // (FRAMES * ROWS) * ROWS + column % ROWS
    late = jnp.zeros((ROWS, LANES), jnp.int32)
    for e in range(elems):
        late = jnp.where(column == e, delay_ref[e], late)
    late = jnp.concatenate([late] * (subbands // ROWS), axis=0)
    cos_late, sin_late = cosine(wanted * late, chan), sine(wanted * late, chan)

    def arrive(k):
        volt_copies[k].wait()
        if k + ahead < chunks:
            volt_copies[k + ahead].start()
        if k == parts:
            basis_copy.start()
            weight_copy.start()

    span = FRAMES * ROWS
    inside = lane // span
    chosen = [None, None]
    products = {}

    def pick(g, r):
        products[g, r] = lax.dot_general(
            pick_ref[r],
            wave_ref[r, pl.ds(g * span, span)],
            NT,
            preferred_element_type=jnp.float32,
        )

    def join(g):
        both = sum(products[g, r] for r in range(parts))
        if span < LANES:
            both = jnp.concatenate(
                [both, jnp.zeros((both.shape[0], LANES - span), jnp.float32)], axis=1
            )
        if g:
            both = pltpu.roll(both, g * span, 1)
        for i in range(2):
            piece = both[i * subbands : (i + 1) * subbands]
            chosen[i] = piece if chosen[i] is None else jnp.where(inside == g, piece, chosen[i])

    proto_copy.wait()
    wide_ref[...] = proto_ref[...].astype(jnp.float32)
    pairs = per // 2
    plan = turn_plan(order[0][0], delay_ref)
    turn_pair(0, 0, plan, wide_ref, spun_ref, coef_ref)
    todo = [[] for _ in order]
    for n in range(groups):
        for p in range(n == 0, pairs):
            ahead_by = parts if n > 1 else 1
            spread = p * ahead_by // pairs
            todo[max(0, n * parts - ahead_by) + spread].append((n, p))
    plans = {0: plan}
    for k, (g, r) in enumerate(order):
        arrive(k)
        n = k // parts
        early = plans[n][1].astype(jnp.int32)
        early = jnp.concatenate([early, jnp.zeros_like(early)], axis=1) != 0
        if k:
            pick(*order[k - 1])
        if k >= parts and r == 1:
            join(order[k - parts][0])
        for p in range(pairs):
            filter_pair(g, r, k, p, n % 2, early, volt_ref, coef_ref, wave_ref)
            if todo[k]:
                unit, q = todo[k].pop(0)
                if unit not in plans:
                    plans[unit] = turn_plan(order[unit * parts][0], delay_ref)
                turn_pair(q, unit % 2, plans[unit], wide_ref, spun_ref, coef_ref)
    pick(*order[-1])
    join(order[-1][0])
    real = chosen[0] * cos_late - chosen[1] * sin_late
    imag = chosen[1] * cos_late + chosen[0] * sin_late
    for c in range(nchan):
        part = slice(c * block, (c + 1) * block)
        send_ref[c] = jnp.concatenate([real[part], imag[part]], axis=0).astype(jnp.bfloat16)

    pl.semaphore_wait(barrier, count - 1)
    my_set = me // gather

    def send(other, c):
        pltpu.make_async_remote_copy(
            src_ref=send_ref.at[c],
            dst_ref=recv_ref.at[me],
            send_sem=send_sem,
            recv_sem=recv_sem.at[my_set],
            device_id=other,
            device_id_type=LOGICAL,
        ).start()

    each_partner(send)
    recv_ref[me] = send_ref[chan_at]

    lanes = chan // RADIX
    wave = [wave_ref[r] for r in range(2)]
    split_wave = [
        tuple(wave[r][:, a * lanes : (a + 1) * lanes].astype(jnp.float32) for r in range(2))
        for a in range(RADIX)
    ]
    classes = eight_points(split_wave)
    basis_copy.wait()
    powers = []
    for c in range(RADIX):
        mixed = jnp.concatenate(classes[c], axis=1).astype(jnp.bfloat16)
        spec = jnp.dot(mixed, basis_ref[c], preferred_element_type=jnp.float32)
        both = spec[:, :lanes] * spec[:, :lanes] + spec[:, lanes:] * spec[:, lanes:]
        totals = []
        for g in range(groups):
            tiles = [
                both[(g * FRAMES + f) * ROWS : (g * FRAMES + f + 1) * ROWS] for f in range(FRAMES)
            ]
            totals.append(sum(tiles[1:], tiles[0]))
        powers.append(jnp.concatenate(totals, axis=0) * (1.0 / FRAMES))
    wide = lanes // RADIX
    at = lax.broadcasted_iota(jnp.int32, (elems, lanes), 1)
    mixed = []
    for e in range(RADIX):
        piece = None
        for c in range(RADIX):
            shift = (wide * (c - e)) % lanes
            moved = pltpu.roll(powers[c], shift, 1) if shift else powers[c]
            piece = moved if piece is None else jnp.where(at // wide == c, moved, piece)
        mixed.append(piece)
    mixed = jnp.concatenate(mixed, axis=0).astype(jnp.bfloat16)
    down = lax.broadcasted_iota(jnp.int32, (lanes, lanes), 0)
    over = lax.broadcasted_iota(jnp.int32, (lanes, lanes), 1)
    back = (over == (down % wide) * RADIX + down // wide).astype(jnp.float32)
    final = jnp.dot(mixed, back.astype(jnp.bfloat16), preferred_element_type=jnp.float32)
    for e in range(RADIX):
        power_ref[:, e * lanes : (e + 1) * lanes] = final[e * elems : (e + 1) * elems].astype(
            jnp.bfloat16
        )

    beams = raw_ref.shape[0]
    weight_rows, total = weight_ref.shape
    wide_beams = turned_ref.shape[1] // block
    down = lax.broadcasted_iota(jnp.int32, (weight_rows, block * wide_beams), 0)
    over = lax.broadcasted_iota(jnp.int32, (weight_rows, block * wide_beams), 1)
    target = down % block * wide_beams + down // block % 2 * (wide_beams // 2)
    sort = (over == target + down // (2 * block)).astype(jnp.float32).astype(jnp.bfloat16)
    weight_copy.wait()
    step = min(8, beams)
    for i in range(0, beams, step):
        piece = raw_ref[i : i + step].reshape(step * 2 * block, raw_ref.shape[3])
        weight_ref[2 * block * i : 2 * block * (i + step)] = piece
    fan = LANES // elems

    def turn_weights(q, carry):
        depth = min(total, 8 * LANES)
        where = pl.multiple_of(q * depth, depth)
        turned = lax.dot_general(
            weight_ref[:, pl.ds(where, depth)], sort, TN, preferred_element_type=jnp.float32
        )
        for z in range(0, depth, LANES):
            tiles = [
                turned[z + (i * groups + g) * ROWS : z + (i * groups + g + 1) * ROWS]
                for g in range(groups)
                for i in range(fan)
            ]
            turned_ref[pl.ds(pl.multiple_of(where + z, LANES), LANES), :] = jnp.concatenate(
                tiles, axis=0
            ).astype(jnp.bfloat16)
        return carry

    if total <= 8 * LANES:
        turn_weights(0, 0)
    else:
        lax.fori_loop(0, total // (8 * LANES), turn_weights, 0)

    sets = count // gather
    place_at = lax.broadcasted_iota(jnp.int32, (2 * block, LANES), 1) // ROWS % fan
    low_row = lax.broadcasted_iota(jnp.int32, (2 * block, wide_beams), 0)

    def take(k, carry):
        which = jnp.where(near_start, k, sets - 1 - k)
        first = which * gather

        def arrived(n):
            some = recv_ref.at[pl.ds(0, n)]
            pltpu.make_async_copy(some, some, recv_sem.at[which]).wait()

        pl.when(which == my_set)(lambda: arrived(gather - 1))
        pl.when(which != my_set)(lambda: arrived(gather))
        pieces = [[] for _ in range(FRAMES)]
        for q in range(gather // fan):
            tiles = [recv_ref[first + q * fan + i].astype(jnp.float32) for i in range(fan)]
            for f in range(FRAMES):
                piece = None
                for i in range(fan):
                    shift = (ROWS * (i - f)) % LANES
                    moved = pltpu.roll(tiles[i], shift, 1) if shift else tiles[i]
                    piece = moved if piece is None else jnp.where(place_at == i, moved, piece)
                pieces[f].append(piece)
        picked = jnp.concatenate(
            [jnp.concatenate(p, axis=1) for p in pieces], axis=0
        ).astype(jnp.bfloat16)
        depth = gather * elems
        where = pl.multiple_of(which * depth, depth)
        product = jnp.dot(
            picked, turned_ref[pl.ds(where, depth), :], preferred_element_type=jnp.float32
        )
        out = []
        for f in range(FRAMES):
            tile = product[2 * block * f : 2 * block * (f + 1)]
            piece = tile[:, :wide_beams]
            for s in range(1, block):
                piece = jnp.where(
                    low_row % block == s, tile[:, s * wide_beams : (s + 1) * wide_beams], piece
                )
            out.append(piece if carry is None else carry[f] + piece)
        return tuple(out)

    if sets <= 8:
        sums = None
        for k in range(sets):
            sums = take(k, sums)
    else:
        zero = jnp.zeros((2 * block, wide_beams), jnp.float32)
        sums = lax.fori_loop(0, sets, take, (zero,) * FRAMES)
    for f in range(FRAMES):
        other = pltpu.roll(pltpu.roll(sums[f], wide_beams // 2, 1), block, 0)
        out = sums[f] + jnp.where(low_row < block, -other, other)
        for p in range(2):
            for s in range(block):
                at = p * block + s
                beam_ref[p, pl.ds(s * FRAMES + f, 1), :] = out[at : at + 1, :beams]

    sent = recv_ref.at[pl.ds(0, count - 1)]
    pltpu.make_async_copy(sent, sent, send_sem).wait()


def class_basis(chan):
    lanes = chan // RADIX
    b = np.arange(lanes)[:, None]
    d = np.arange(lanes)[None, :]
    out = []
    for c in range(RADIX):
        angle = 2.0 * np.pi / chan * (b * (c + RADIX * d) % chan)
        cos, sin = np.cos(angle) * chan**-0.5, np.sin(angle) * chan**-0.5
        out.append(np.block([[cos, -sin], [sin, cos]]))
    return jnp.asarray(np.stack(out), jnp.bfloat16)


def deliver_kernel(power_from, beam_from, power_to, beam_to, sems):
    copies = [
        pltpu.make_async_copy(power_from, power_to, sems.at[0]),
        pltpu.make_async_copy(beam_from, beam_to, sems.at[1]),
    ]
    for copy in copies:
        copy.start()
    for copy in copies:
        copy.wait()


def on_device(nelem, nchan, voltages, delays, prototype, subband_map, beam_weights):
    parts, elems, samples = voltages.shape
    taps, chan = prototype.shape
    beams, _, block, total = beam_weights.shape
    basis = class_basis(chan)
    count = nelem * nchan
    chunks = parts * elems // ROWS
    gather = 8
    wide_beams = max(LANES, 2 * beams)
    out_shape = [
        jax.ShapeDtypeStruct((elems, chan), jnp.bfloat16),
        jax.ShapeDtypeStruct((2, block * FRAMES, beams), jnp.float32),
    ]
    power, beam = pl.pallas_call(
        functools.partial(main_kernel, nelem, nchan, gather),
        in_specs=[pl.BlockSpec(memory_space=pltpu.HBM)] * 6,
        out_specs=[pl.BlockSpec(memory_space=pltpu.VMEM)] * 2,
        out_shape=[pltpu.VMEM(o.shape, o.dtype) for o in out_shape],
        scratch_shapes=[
            pltpu.SMEM(delays.shape, jnp.int32),
            pltpu.SMEM(subband_map.shape, jnp.int32),
            pltpu.VMEM((chunks, ROWS, samples), jnp.bfloat16),
            pltpu.VMEM((taps, chan), jnp.bfloat16),
            pltpu.VMEM(beam_weights.shape, jnp.bfloat16),
            pltpu.VMEM(basis.shape, jnp.bfloat16),
            pltpu.VMEM((taps, chan), jnp.float32),
            pltpu.VMEM((taps, ROWS, chan), jnp.float32),
            pltpu.VMEM((2, taps, ROWS, chan), jnp.bfloat16),
            pltpu.VMEM((2, 2 * subband_map.shape[0], chan), jnp.bfloat16),
            pltpu.VMEM((parts, FRAMES * elems, chan), jnp.bfloat16),
            pltpu.VMEM((beams * 2 * block, total), jnp.bfloat16),
            pltpu.VMEM((total, block * wide_beams), jnp.bfloat16),
            pltpu.VMEM((nchan, 2 * block, FRAMES * elems), jnp.bfloat16),
            pltpu.VMEM((count, 2 * block, FRAMES * elems), jnp.bfloat16),
            pltpu.SemaphoreType.DMA((5,)),
            pltpu.SemaphoreType.DMA((chunks,)),
            pltpu.SemaphoreType.DMA,
            pltpu.SemaphoreType.DMA((count // gather,)),
        ],
        compiler_params=pltpu.CompilerParams(
            collective_id=0, has_side_effects=True, vmem_limit_bytes=66_400_000
        ),
    )(delays, subband_map, voltages, prototype, beam_weights, basis)
    return pl.pallas_call(
        deliver_kernel,
        in_specs=[pl.BlockSpec(memory_space=pl.ANY)] * 2,
        out_specs=[pl.BlockSpec(memory_space=pl.ANY)] * 2,
        out_shape=out_shape,
        scratch_shapes=[pltpu.SemaphoreType.DMA((2,))],
        compiler_params=pltpu.CompilerParams(vmem_limit_bytes=2**20),
    )(power, beam)


def solution(mesh):
    return jax.shard_map(
        functools.partial(on_device, mesh.shape["elem"], mesh.shape["chan"]),
        mesh=mesh,
        in_specs=(
            P(None, ("elem", "chan"), None),
            P(("elem", "chan")),
            P(),
            P(),
            P("elem", None, "chan", None),
        ),
        out_specs=(P(("elem", "chan"), None), P(None, "chan", "elem")),
        check_vma=False,
    )
```

```python
import functools
import math

import jax
import jax.numpy as jnp
import numpy as np
from jax import lax
from jax.experimental import pallas as pl
from jax.experimental.pallas import tpu as pltpu
from jax.sharding import PartitionSpec as P

FRAMES = 4
LANES = 128
ROWS = 8
RADIX = 8
LOGICAL = pl.DeviceIdType.LOGICAL
NT = (((1,), (1,)), ((), ()))
TN = (((0,), (0,)), ((), ()))


def cosine(turns, chan):
    y = jnp.abs((turns & (chan - 1)) - chan // 2) - chan // 4
    x = y.astype(jnp.float32) * (2.0 * math.pi / chan)
    s = x * x
    poly = 1.0 / 362880 - s * (1.0 / 39916800)
    poly = -1.0 / 5040 + s * poly
    poly = 1.0 / 120 + s * poly
    poly = -1.0 / 6 + s * poly
    return x + x * s * poly


def sine(turns, chan):
    return cosine(turns + 3 * (chan // 4), chan)


def eight_points(x):
    def add(a, b):
        return (a[0] + b[0], a[1] + b[1])

    def sub(a, b):
        return (a[0] - b[0], a[1] - b[1])

    def minus_i(a):
        return (a[1], -a[0])

    def four(v):
        a, b = add(v[0], v[2]), sub(v[0], v[2])
        c, d = add(v[1], v[3]), minus_i(sub(v[1], v[3]))
        return [add(a, c), add(b, d), sub(a, c), sub(b, d)]

    root = math.sqrt(0.5)
    even = four([add(x[a], x[a + 4]) for a in range(4)])
    d = [sub(x[a], x[a + 4]) for a in range(4)]
    d1 = ((d[1][0] + d[1][1]) * root, (d[1][1] - d[1][0]) * root)
    d3 = ((d[3][1] - d[3][0]) * root, (-d[3][0] - d[3][1]) * root)
    odd = four([d[0], d1, minus_i(d[2]), d3])
    out = []
    for e, o in zip(even, odd):
        out += [e, o]
    return out


def turn_plan(group, delay_ref):
    lane = lax.broadcasted_iota(jnp.int32, (ROWS, LANES), 1)
    sub = lax.broadcasted_iota(jnp.int32, (ROWS, LANES), 0)
    shift = jnp.zeros((ROWS, LANES), jnp.int32)
    for i in range(ROWS):
        shift = jnp.where(sub == i, delay_ref[group * ROWS + i], shift)
    return (lane - shift) & (LANES - 1), lane < shift


def turn_pair(pair, slot, plan, proto_ref, turned_ref, coef_ref):
    index, early = plan
    taps, chan = proto_ref.shape
    per = chan // LANES
    first, last = 2 * pair, min(2 * pair + 2, per - 1)
    fresh = [*range(first, last), per - 1] if pair == 0 else range(first, last)
    for t in range(taps):
        for j in fresh:
            where = pl.ds(j * LANES, LANES)
            value = jnp.broadcast_to(proto_ref[pl.ds(t, 1), where], (ROWS, LANES))
            turned_ref[t, :, where] = jnp.take_along_axis(
                value, index, axis=1, mode="promise_in_bounds"
            )
        near = [
            turned_ref[t, :, pl.ds((first + i) % per * LANES, LANES)] for i in (-1, 0, 1)
        ]
        coef_ref[slot, t, :, pl.ds(first * LANES, 2 * LANES)] = jnp.concatenate(
            [jnp.where(early, near[0], near[1]), jnp.where(early, near[1], near[2])], axis=1
        ).astype(jnp.bfloat16)


def filter_pair(group, part, chunk, pair, slot, early, volt_ref, coef_ref, wave_ref):
    _, taps, _, chan = coef_ref.shape
    blocks = FRAMES + taps - 1
    wide = 2 * LANES

    def column(b, size):
        return volt_ref[chunk, part, :, pl.ds(b * chan + pair * wide, size)]

    held = [column(b, wide) for b in range(blocks)]
    if pair == 0:
        last = jnp.concatenate([column(blocks, LANES), held[-1][:, LANES:]], axis=1)
        held = [
            jnp.where(early, nxt, now) for now, nxt in zip(held, [*held[1:], last])
        ]
    stacks = [[] for _ in range(FRAMES)]
    for t in range(taps):
        coef = coef_ref[slot, t, :, pl.ds(pair * wide, wide)]
        for f in range(FRAMES):
            level, term = 0, coef * held[f + t]
            while stacks[f] and stacks[f][-1][0] == level:
                level, term = level + 1, stacks[f].pop()[1] + term
            stacks[f].append((level, term))
    for f in range(FRAMES):
        total = stacks[f].pop()[1]
        while stacks[f]:
            total = stacks[f].pop()[1] + total
        where = pl.ds((group * FRAMES + f) * ROWS, ROWS)
        wave_ref[part, where, pl.ds(pair * wide, wide)] = total


def main_kernel(
    nelem,
    nchan,
    gather,
    delay_hbm,
    map_hbm,
    volt_hbm,
    proto_hbm,
    weight_hbm,
    basis_hbm,
    power_ref,
    beam_ref,
    delay_ref,
    map_ref,
    volt_ref,
    proto_ref,
    raw_ref,
    basis_ref,
    wide_ref,
    spun_ref,
    coef_ref,
    pick_ref,
    wave_ref,
    weight_ref,
    turned_ref,
    send_ref,
    recv_ref,
    send_sem,
    recv_sem,
):
    parts, wave_rows, chan = wave_ref.shape
    groups = volt_ref.shape[0]
    elems = groups * ROWS
    taps = proto_ref.shape[0]
    per = chan // LANES
    count = nelem * nchan
    elem_at, chan_at = lax.axis_index("elem"), lax.axis_index("chan")
    me = elem_at * nchan + chan_at
    near_start = elem_at < nelem // 2
    barrier = pltpu.get_barrier_semaphore()

    def each_partner(act):
        def row(k, carry):
            first = jnp.where(near_start, nelem - 1 - k, k) * nchan
            for c in range(nchan):

                @pl.when(first + c != me)
                def _():
                    act(first + c, c)

            return carry

        if count <= 64:
            for k in range(nelem):
                row(k, 0)
        else:
            lax.fori_loop(0, nelem, row, 0)

    subbands = map_ref.shape[0]
    block = subbands // nchan
    my_set = me // gather
    beams = raw_ref.shape[0]
    weight_rows, total = weight_ref.shape
    wide_beams = turned_ref.shape[1] // block
    fan = LANES // elems

    def front(local_sem, volt_sem):
        order = [*range(1, groups), 0]
        map_copy = pltpu.make_async_copy(map_hbm, map_ref, local_sem.at[0])
        proto_copy = pltpu.make_async_copy(proto_hbm, proto_ref, local_sem.at[1])
        delay_copy = pltpu.make_async_copy(delay_hbm, delay_ref, local_sem.at[2])
        basis_copy = pltpu.make_async_copy(basis_hbm, basis_ref, local_sem.at[3])
        weight_copy = pltpu.make_async_copy(weight_hbm, raw_ref, local_sem.at[4])
        volt_copies = [
            pltpu.make_async_copy(
                volt_hbm.at[r, pl.ds(order[0] * ROWS, ROWS)], volt_ref.at[0, r], volt_sem.at[r]
            )
            for r in range(parts)
        ]
        for k, g in enumerate(order[1:]):
            volt_copies.append(
                pltpu.make_async_copy(
                    volt_hbm.at[:, pl.ds(g * ROWS, ROWS)],
                    volt_ref.at[k + 1],
                    volt_sem.at[k + parts],
                )
            )
        proto_copy.start()
        delay_copy.start()
        map_copy.start()
        for copy in volt_copies[:parts]:
            copy.start()

        def greet(other, c):
            pl.semaphore_signal(barrier, inc=1, device_id=other, device_id_type=LOGICAL)

        each_partner(greet)
        for copy in volt_copies[parts:]:
            copy.start()

        map_copy.wait()
        delay_copy.wait()
        proto_copy.wait()
        wide_ref[...] = proto_ref[...].astype(jnp.float32)
        pairs = per // 2
        plans = [turn_plan(order[0], delay_ref)]
        turn_pair(0, 0, plans[0], wide_ref, spun_ref, coef_ref)
        row = lax.broadcasted_iota(jnp.int32, (subbands, LANES), 0)
        lane = lax.broadcasted_iota(jnp.int32, (subbands, LANES), 1)
        wanted = jnp.zeros((subbands, LANES), jnp.int32)
        for s in range(subbands):
            wanted = jnp.where(row == s, map_ref[s], wanted)
        scale = chan**-0.5
        cos, sin = cosine(wanted * lane, chan) * scale, sine(wanted * lane, chan) * scale
        cos_step, sin_step = cosine(wanted * LANES, chan), sine(wanted * LANES, chan)
        for j in range(per):
            if j:
                cos, sin = cos * cos_step - sin * sin_step, sin * cos_step + cos * sin_step
            where = pl.ds(j * LANES, LANES)
            pick_ref[0, pl.ds(0, subbands), where] = cos.astype(jnp.bfloat16)
            pick_ref[0, pl.ds(subbands, subbands), where] = (-sin).astype(jnp.bfloat16)
            pick_ref[1, pl.ds(0, subbands), where] = sin.astype(jnp.bfloat16)
            pick_ref[1, pl.ds(subbands, subbands), where] = cos.astype(jnp.bfloat16)
        column = lax.broadcasted_iota(jnp.int32, (ROWS, LANES), 1)
        column = column // (FRAMES * ROWS) * ROWS + column % ROWS
        late = jnp.zeros((ROWS, LANES), jnp.int32)
        for e in range(elems):
            late = jnp.where(column == e, delay_ref[e], late)
        late = jnp.concatenate([late] * (subbands // ROWS), axis=0)
        cos_late, sin_late = cosine(wanted * late, chan), sine(wanted * late, chan)

        span = FRAMES * ROWS

        def pick(first, size):
            both = sum(
                lax.dot_general(
                    pick_ref[r],
                    wave_ref[r, pl.ds(first, size)],
                    NT,
                    preferred_element_type=jnp.float32,
                )
                for r in range(parts)
            )
            both = [both]
            if first:
                both = [jnp.zeros((2 * subbands, first), jnp.float32), *both]
            if first + size < LANES:
                both.append(jnp.zeros((2 * subbands, LANES - first - size), jnp.float32))
            return jnp.concatenate(both, axis=1)

        units = parts * pairs
        todo = [[] for _ in range(groups * units)]
        for p in range(1, pairs):
            todo[p - 1].append((0, p))
        for n in range(1, groups):
            for p in range(pairs):
                todo[n * units + p - 1].append((n, p))
        both = None
        for n, g in enumerate(order):
            volt_copies[n + parts - 1 if n else 0].wait()
            if n == 1:
                basis_copy.start()
                weight_copy.start()
            if n + 1 < groups:
                plans.append(turn_plan(order[n + 1], delay_ref))
            early = plans[n][1].astype(jnp.int32)
            early = jnp.concatenate([early, jnp.zeros_like(early)], axis=1) != 0
            if n == groups - 2:
                chosen = pick(span, n * span)
            if n == groups - 1:
                chosen = chosen + pick(n * span, span)
            for r in range(parts):
                if n == 0 and r:
                    volt_copies[r].wait()
                for p in range(pairs):
                    filter_pair(g, r, n, p, n % 2, early, volt_ref, coef_ref, wave_ref)
                    for unit, q in todo[n * units + r * pairs + p]:
                        turn_pair(q, unit % 2, plans[unit], wide_ref, spun_ref, coef_ref)
        final = pick(0, span)
        chosen = jnp.where(lax.broadcasted_iota(jnp.int32, final.shape, 1) < span, final, chosen)
        real = chosen[:subbands] * cos_late - chosen[subbands:] * sin_late
        imag = chosen[subbands:] * cos_late + chosen[:subbands] * sin_late
        for c in range(nchan):
            part = slice(c * block, (c + 1) * block)
            send_ref[c] = jnp.concatenate([real[part], imag[part]], axis=0).astype(jnp.bfloat16)

        pl.semaphore_wait(barrier, count - 1)

        def send(other, c):
            pltpu.make_async_remote_copy(
                src_ref=send_ref.at[c],
                dst_ref=recv_ref.at[me],
                send_sem=send_sem,
                recv_sem=recv_sem.at[my_set],
                device_id=other,
                device_id_type=LOGICAL,
            ).start()

        each_partner(send)
        recv_ref[me] = send_ref[chan_at]

        lanes = chan // RADIX
        wave = [wave_ref[r] for r in range(2)]
        split_wave = [
            tuple(wave[r][:, a * lanes : (a + 1) * lanes].astype(jnp.float32) for r in range(2))
            for a in range(RADIX)
        ]
        classes = eight_points(split_wave)
        basis_copy.wait()
        powers = []
        for c in range(RADIX):
            mixed = jnp.concatenate(classes[c], axis=1).astype(jnp.bfloat16)
            spec = jnp.dot(mixed, basis_ref[c], preferred_element_type=jnp.float32)
            both = spec[:, :lanes] * spec[:, :lanes] + spec[:, lanes:] * spec[:, lanes:]
            totals = []
            for g in range(groups):
                tiles = [
                    both[(g * FRAMES + f) * ROWS : (g * FRAMES + f + 1) * ROWS] for f in range(FRAMES)
                ]
                totals.append(sum(tiles[1:], tiles[0]))
            powers.append(jnp.concatenate(totals, axis=0) * (1.0 / FRAMES))
        wide = lanes // RADIX
        at = lax.broadcasted_iota(jnp.int32, (elems, lanes), 1)
        mixed = []
        for e in range(RADIX):
            piece = None
            for c in range(RADIX):
                shift = (wide * (c - e)) % lanes
                moved = pltpu.roll(powers[c], shift, 1) if shift else powers[c]
                piece = moved if piece is None else jnp.where(at // wide == c, moved, piece)
            mixed.append(piece)
        mixed = jnp.concatenate(mixed, axis=0).astype(jnp.bfloat16)
        down = lax.broadcasted_iota(jnp.int32, (lanes, lanes), 0)
        over = lax.broadcasted_iota(jnp.int32, (lanes, lanes), 1)
        back = (over == (down % wide) * RADIX + down // wide).astype(jnp.float32)
        final = jnp.dot(mixed, back.astype(jnp.bfloat16), preferred_element_type=jnp.float32)
        for e in range(RADIX):
            power_ref[:, e * lanes : (e + 1) * lanes] = final[e * elems : (e + 1) * elems].astype(
                jnp.bfloat16
            )

        down = lax.broadcasted_iota(jnp.int32, (weight_rows, block * wide_beams), 0)
        over = lax.broadcasted_iota(jnp.int32, (weight_rows, block * wide_beams), 1)
        target = down % block * wide_beams + down // block % 2 * (wide_beams // 2)
        sort = (over == target + down // (2 * block)).astype(jnp.float32).astype(jnp.bfloat16)
        weight_copy.wait()
        step = min(8, beams)
        for i in range(0, beams, step):
            piece = raw_ref[i : i + step].reshape(step * 2 * block, raw_ref.shape[3])
            weight_ref[2 * block * i : 2 * block * (i + step)] = piece

        def turn_weights(q, carry):
            depth = min(total, 8 * LANES)
            where = pl.multiple_of(q * depth, depth)
            turned = lax.dot_general(
                weight_ref[:, pl.ds(where, depth)], sort, TN, preferred_element_type=jnp.float32
            )
            for z in range(0, depth, LANES):
                tiles = [
                    turned[z + (i * groups + g) * ROWS : z + (i * groups + g + 1) * ROWS]
                    for g in range(groups)
                    for i in range(fan)
                ]
                turned_ref[pl.ds(pl.multiple_of(where + z, LANES), LANES), :] = jnp.concatenate(
                    tiles, axis=0
                ).astype(jnp.bfloat16)
            return carry

        if total <= 8 * LANES:
            turn_weights(0, 0)
        else:
            lax.fori_loop(0, total // (8 * LANES), turn_weights, 0)

    pl.run_scoped(
        front, pltpu.SemaphoreType.DMA((5,)), pltpu.SemaphoreType.DMA((groups + parts - 1,))
    )

    sets = count // gather
    place_at = lax.broadcasted_iota(jnp.int32, (2 * block, LANES), 1) // ROWS % fan
    low_row = lax.broadcasted_iota(jnp.int32, (2 * block, wide_beams), 0)

    def take(k, carry):
        which = jnp.where(near_start, k, sets - 1 - k)
        first = which * gather

        def arrived(n):
            some = recv_ref.at[pl.ds(0, n)]
            pltpu.make_async_copy(some, some, recv_sem.at[which]).wait()

        pl.when(which == my_set)(lambda: arrived(gather - 1))
        pl.when(which != my_set)(lambda: arrived(gather))
        pieces = [[] for _ in range(FRAMES)]
        for q in range(gather // fan):
            tiles = [recv_ref[first + q * fan + i].astype(jnp.float32) for i in range(fan)]
            for f in range(FRAMES):
                piece = None
                for i in range(fan):
                    shift = (ROWS * (i - f)) % LANES
                    moved = pltpu.roll(tiles[i], shift, 1) if shift else tiles[i]
                    piece = moved if piece is None else jnp.where(place_at == i, moved, piece)
                pieces[f].append(piece)
        picked = jnp.concatenate(
            [jnp.concatenate(p, axis=1) for p in pieces], axis=0
        ).astype(jnp.bfloat16)
        depth = gather * elems
        where = pl.multiple_of(which * depth, depth)
        product = jnp.dot(
            picked, turned_ref[pl.ds(where, depth), :], preferred_element_type=jnp.float32
        )
        out = []
        for f in range(FRAMES):
            tile = product[2 * block * f : 2 * block * (f + 1)]
            piece = tile[:, :wide_beams]
            for s in range(1, block):
                piece = jnp.where(
                    low_row % block == s, tile[:, s * wide_beams : (s + 1) * wide_beams], piece
                )
            out.append(piece if carry is None else carry[f] + piece)
        return tuple(out)

    if sets <= 8:
        sums = None
        for k in range(sets):
            sums = take(k, sums)
    else:
        zero = jnp.zeros((2 * block, wide_beams), jnp.float32)
        sums = lax.fori_loop(0, sets, take, (zero,) * FRAMES)
    for f in range(FRAMES):
        other = pltpu.roll(pltpu.roll(sums[f], wide_beams // 2, 1), block, 0)
        out = sums[f] + jnp.where(low_row < block, -other, other)
        for p in range(2):
            for s in range(block):
                at = p * block + s
                beam_ref[p, pl.ds(s * FRAMES + f, 1), :] = out[at : at + 1, :beams]

    sent = recv_ref.at[pl.ds(0, count - 1)]
    pltpu.make_async_copy(sent, sent, send_sem).wait()


def class_basis(chan):
    lanes = chan // RADIX
    b = np.arange(lanes)[:, None]
    d = np.arange(lanes)[None, :]
    out = []
    for c in range(RADIX):
        angle = 2.0 * np.pi / chan * (b * (c + RADIX * d) % chan)
        cos, sin = np.cos(angle) * chan**-0.5, np.sin(angle) * chan**-0.5
        out.append(np.block([[cos, -sin], [sin, cos]]))
    return jnp.asarray(np.stack(out), jnp.bfloat16)


def deliver_kernel(power_from, beam_from, power_to, beam_to, sems):
    copies = [
        pltpu.make_async_copy(power_from, power_to, sems.at[0]),
        pltpu.make_async_copy(beam_from, beam_to, sems.at[1]),
    ]
    for copy in copies:
        copy.start()
    for copy in copies:
        copy.wait()


def on_device(nelem, nchan, voltages, delays, prototype, subband_map, beam_weights):
    parts, elems, samples = voltages.shape
    taps, chan = prototype.shape
    beams, _, block, total = beam_weights.shape
    basis = class_basis(chan)
    count = nelem * nchan
    gather = 8
    wide_beams = max(LANES, 2 * beams)
    out_shape = [
        jax.ShapeDtypeStruct((elems, chan), jnp.bfloat16),
        jax.ShapeDtypeStruct((2, block * FRAMES, beams), jnp.float32),
    ]
    power, beam = pl.pallas_call(
        functools.partial(main_kernel, nelem, nchan, gather),
        in_specs=[pl.BlockSpec(memory_space=pltpu.HBM)] * 6,
        out_specs=[pl.BlockSpec(memory_space=pltpu.VMEM)] * 2,
        out_shape=[pltpu.VMEM(o.shape, o.dtype) for o in out_shape],
        scratch_shapes=[
            pltpu.SMEM(delays.shape, jnp.int32),
            pltpu.SMEM(subband_map.shape, jnp.int32),
            pltpu.VMEM((elems // ROWS, parts, ROWS, samples), jnp.bfloat16),
            pltpu.VMEM((taps, chan), jnp.bfloat16),
            pltpu.VMEM(beam_weights.shape, jnp.bfloat16),
            pltpu.VMEM(basis.shape, jnp.bfloat16),
            pltpu.VMEM((taps, chan), jnp.float32),
            pltpu.VMEM((taps, ROWS, chan), jnp.float32),
            pltpu.VMEM((2, taps, ROWS, chan), jnp.bfloat16),
            pltpu.VMEM((2, 2 * subband_map.shape[0], chan), jnp.bfloat16),
            pltpu.VMEM((parts, FRAMES * elems, chan), jnp.bfloat16),
            pltpu.VMEM((beams * 2 * block, total), jnp.bfloat16),
            pltpu.VMEM((total, block * wide_beams), jnp.bfloat16),
            pltpu.VMEM((nchan, 2 * block, FRAMES * elems), jnp.bfloat16),
            pltpu.VMEM((count, 2 * block, FRAMES * elems), jnp.bfloat16),
            pltpu.SemaphoreType.DMA,
            pltpu.SemaphoreType.DMA((count // gather,)),
        ],
        compiler_params=pltpu.CompilerParams(
            collective_id=0, has_side_effects=True, vmem_limit_bytes=66_400_000
        ),
    )(delays, subband_map, voltages, prototype, beam_weights, basis)
    return pl.pallas_call(
        deliver_kernel,
        in_specs=[pl.BlockSpec(memory_space=pl.ANY)] * 2,
        out_specs=[pl.BlockSpec(memory_space=pl.ANY)] * 2,
        out_shape=out_shape,
        scratch_shapes=[pltpu.SemaphoreType.DMA((2,))],
        compiler_params=pltpu.CompilerParams(vmem_limit_bytes=2**20),
    )(power, beam)


def solution(mesh):
    return jax.shard_map(
        functools.partial(on_device, mesh.shape["elem"], mesh.shape["chan"]),
        mesh=mesh,
        in_specs=(
            P(None, ("elem", "chan"), None),
            P(("elem", "chan")),
            P(),
            P(),
            P("elem", None, "chan", None),
        ),
        out_specs=(P(("elem", "chan"), None), P(None, "chan", "elem")),
        check_vma=False,
    )
```

```python
import functools
import math

import jax
import jax.numpy as jnp
import numpy as np
from jax import lax
from jax.experimental import pallas as pl
from jax.experimental.pallas import tpu as pltpu
from jax.sharding import PartitionSpec as P

FRAMES = 4
LANES = 128
ROWS = 8
RADIX = 8
LOGICAL = pl.DeviceIdType.LOGICAL
NT = (((1,), (1,)), ((), ()))
TN = (((0,), (0,)), ((), ()))


def cosine(turns, chan):
    y = jnp.abs((turns & (chan - 1)) - chan // 2) - chan // 4
    x = y.astype(jnp.float32) * (2.0 * math.pi / chan)
    s = x * x
    poly = 1.0 / 362880 - s * (1.0 / 39916800)
    poly = -1.0 / 5040 + s * poly
    poly = 1.0 / 120 + s * poly
    poly = -1.0 / 6 + s * poly
    return x + x * s * poly


def sine(turns, chan):
    return cosine(turns + 3 * (chan // 4), chan)


def eight_points(x):
    def add(a, b):
        return (a[0] + b[0], a[1] + b[1])

    def sub(a, b):
        return (a[0] - b[0], a[1] - b[1])

    def minus_i(a):
        return (a[1], -a[0])

    def four(v):
        a, b = add(v[0], v[2]), sub(v[0], v[2])
        c, d = add(v[1], v[3]), minus_i(sub(v[1], v[3]))
        return [add(a, c), add(b, d), sub(a, c), sub(b, d)]

    root = math.sqrt(0.5)
    even = four([add(x[a], x[a + 4]) for a in range(4)])
    d = [sub(x[a], x[a + 4]) for a in range(4)]
    d1 = ((d[1][0] + d[1][1]) * root, (d[1][1] - d[1][0]) * root)
    d3 = ((d[3][1] - d[3][0]) * root, (-d[3][0] - d[3][1]) * root)
    odd = four([d[0], d1, minus_i(d[2]), d3])
    out = []
    for e, o in zip(even, odd):
        out += [e, o]
    return out


def turn_plan(group, delay_ref):
    lane = lax.broadcasted_iota(jnp.int32, (ROWS, LANES), 1)
    sub = lax.broadcasted_iota(jnp.int32, (ROWS, LANES), 0)
    shift = jnp.zeros((ROWS, LANES), jnp.int32)
    for i in range(ROWS):
        shift = jnp.where(sub == i, delay_ref[group * ROWS + i], shift)
    return (lane - shift) & (LANES - 1), lane < LANES - shift, lane < shift


def turn_pair(pair, slot, plan, proto_ref, coef_ref):
    index, stay, _ = plan
    taps, chan = proto_ref.shape
    per = chan // LANES
    for t in range(taps):
        near = [
            jnp.broadcast_to(
                proto_ref[pl.ds(t, 1), pl.ds((2 * pair + i) % per * LANES, LANES)], (ROWS, LANES)
            )
            for i in (-1, 0, 1)
        ]
        turned = [
            jnp.take_along_axis(
                jnp.where(stay, near[i + 1], near[i]), index, axis=1, mode="promise_in_bounds"
            )
            for i in range(2)
        ]
        coef_ref[slot, t, :, pl.ds(2 * pair * LANES, 2 * LANES)] = jnp.concatenate(
            turned, axis=1
        ).astype(jnp.bfloat16)


def filter_pair(group, part, chunk, pair, slot, early, volt_ref, coef_ref, wave_ref):
    _, taps, _, chan = coef_ref.shape
    blocks = FRAMES + taps - 1
    wide = 2 * LANES

    def column(b, size):
        return volt_ref[chunk, part, :, pl.ds(b * chan + pair * wide, size)]

    held = [column(b, wide) for b in range(blocks)]
    if pair == 0:
        last = jnp.concatenate([column(blocks, LANES), held[-1][:, LANES:]], axis=1)
        held = [
            jnp.where(early, nxt, now) for now, nxt in zip(held, [*held[1:], last])
        ]
    stacks = [[] for _ in range(FRAMES)]
    for t in range(taps):
        coef = coef_ref[slot, t, :, pl.ds(pair * wide, wide)]
        for f in range(FRAMES):
            level, term = 0, coef * held[f + t]
            while stacks[f] and stacks[f][-1][0] == level:
                level, term = level + 1, stacks[f].pop()[1] + term
            stacks[f].append((level, term))
    for f in range(FRAMES):
        total = stacks[f].pop()[1]
        while stacks[f]:
            total = stacks[f].pop()[1] + total
        where = pl.ds((group * FRAMES + f) * ROWS, ROWS)
        wave_ref[part, where, pl.ds(pair * wide, wide)] = total


def main_kernel(
    nelem,
    nchan,
    gather,
    delay_hbm,
    map_hbm,
    volt_hbm,
    proto_hbm,
    weight_hbm,
    basis_hbm,
    power_ref,
    beam_ref,
    delay_ref,
    map_ref,
    volt_ref,
    proto_ref,
    raw_ref,
    basis_ref,
    wide_ref,
    coef_ref,
    pick_ref,
    wave_ref,
    weight_ref,
    turned_ref,
    send_ref,
    recv_ref,
    send_sem,
    recv_sem,
):
    parts, wave_rows, chan = wave_ref.shape
    groups = volt_ref.shape[0]
    elems = groups * ROWS
    taps = proto_ref.shape[0]
    per = chan // LANES
    count = nelem * nchan
    elem_at, chan_at = lax.axis_index("elem"), lax.axis_index("chan")
    me = elem_at * nchan + chan_at
    near_start = elem_at < nelem // 2
    barrier = pltpu.get_barrier_semaphore()

    def each_partner(act):
        def row(k, carry):
            first = jnp.where(near_start, nelem - 1 - k, k) * nchan
            for c in range(nchan):

                @pl.when(first + c != me)
                def _():
                    act(first + c, c)

            return carry

        if count <= 64:
            for k in range(nelem):
                row(k, 0)
        else:
            lax.fori_loop(0, nelem, row, 0)

    subbands = map_ref.shape[0]
    block = subbands // nchan
    my_set = me // gather
    beams = raw_ref.shape[0]
    weight_rows, total = weight_ref.shape
    wide_beams = turned_ref.shape[1] // block
    fan = LANES // elems

    def front(local_sem, volt_sem):
        order = [*range(1, groups), 0]
        map_copy = pltpu.make_async_copy(map_hbm, map_ref, local_sem.at[0])
        proto_copy = pltpu.make_async_copy(proto_hbm, proto_ref, local_sem.at[1])
        delay_copy = pltpu.make_async_copy(delay_hbm, delay_ref, local_sem.at[2])
        basis_copy = pltpu.make_async_copy(basis_hbm, basis_ref, local_sem.at[3])
        weight_copy = pltpu.make_async_copy(weight_hbm, raw_ref, local_sem.at[4])
        volt_copies = [
            pltpu.make_async_copy(
                volt_hbm.at[r, pl.ds(order[0] * ROWS, ROWS)], volt_ref.at[0, r], volt_sem.at[r]
            )
            for r in range(parts)
        ]
        for k, g in enumerate(order[1:]):
            volt_copies.append(
                pltpu.make_async_copy(
                    volt_hbm.at[:, pl.ds(g * ROWS, ROWS)],
                    volt_ref.at[k + 1],
                    volt_sem.at[k + parts],
                )
            )
        proto_copy.start()
        delay_copy.start()
        map_copy.start()
        for copy in volt_copies[: parts + 1]:
            copy.start()

        def greet(other, c):
            pl.semaphore_signal(barrier, inc=1, device_id=other, device_id_type=LOGICAL)

        each_partner(greet)
        for copy in volt_copies[parts + 1 :]:
            copy.start()

        map_copy.wait()
        delay_copy.wait()
        proto_copy.wait()
        wide_ref[...] = proto_ref[...].astype(jnp.float32)
        pairs = per // 2
        plans = [turn_plan(g, delay_ref) for g in order]
        turn_pair(0, 0, plans[0], wide_ref, coef_ref)
        row = lax.broadcasted_iota(jnp.int32, (subbands, LANES), 0)
        lane = lax.broadcasted_iota(jnp.int32, (subbands, LANES), 1)
        wanted = jnp.zeros((subbands, LANES), jnp.int32)
        for s in range(subbands):
            wanted = jnp.where(row == s, map_ref[s], wanted)
        scale = chan**-0.5
        cos, sin = cosine(wanted * lane, chan) * scale, sine(wanted * lane, chan) * scale
        cos_step, sin_step = cosine(wanted * LANES, chan), sine(wanted * LANES, chan)
        for j in range(per):
            if j:
                cos, sin = cos * cos_step - sin * sin_step, sin * cos_step + cos * sin_step
            where = pl.ds(j * LANES, LANES)
            pick_ref[0, pl.ds(0, subbands), where] = cos.astype(jnp.bfloat16)
            pick_ref[0, pl.ds(subbands, subbands), where] = (-sin).astype(jnp.bfloat16)
            pick_ref[1, pl.ds(0, subbands), where] = sin.astype(jnp.bfloat16)
            pick_ref[1, pl.ds(subbands, subbands), where] = cos.astype(jnp.bfloat16)
        column = lax.broadcasted_iota(jnp.int32, (ROWS, LANES), 1)
        column = column // (FRAMES * ROWS) * ROWS + column % ROWS
        late = jnp.zeros((ROWS, LANES), jnp.int32)
        for e in range(elems):
            late = jnp.where(column == e, delay_ref[e], late)
        late = jnp.concatenate([late] * (subbands // ROWS), axis=0)
        cos_late, sin_late = cosine(wanted * late, chan), sine(wanted * late, chan)

        span = FRAMES * ROWS

        def pick(first, size):
            both = sum(
                lax.dot_general(
                    pick_ref[r],
                    wave_ref[r, pl.ds(first, size)],
                    NT,
                    preferred_element_type=jnp.float32,
                )
                for r in range(parts)
            )
            both = [both]
            if first:
                both = [jnp.zeros((2 * subbands, first), jnp.float32), *both]
            if first + size < LANES:
                both.append(jnp.zeros((2 * subbands, LANES - first - size), jnp.float32))
            return jnp.concatenate(both, axis=1)

        units = parts * pairs
        todo = [[] for _ in range(groups * units)]
        for p in range(1, pairs):
            todo[p - 1].append((0, p))
        for n in range(1, groups):
            for p in range(pairs):
                todo[min(n, 2) * units - pairs + p].append((n, p))
        both = None
        for n, g in enumerate(order):
            if n < groups - 1:
                volt_copies[n + parts - 1 if n else 0].wait()
            if n == groups - 2:
                basis_copy.start()
                weight_copy.start()
            early = plans[n][2].astype(jnp.int32)
            early = jnp.concatenate([early, jnp.zeros_like(early)], axis=1) != 0
            for r in range(parts):
                if n == 0 and r:
                    volt_copies[r].wait()
                if n == groups - 2 and r == parts - 1:
                    volt_copies[-1].wait()
                if n == groups - 2 and r == parts - 1:
                    chosen = pick(span, n * span)
                if n == groups - 1 and r == 0:
                    chosen = chosen + pick(n * span, span)
                for p in range(pairs):
                    filter_pair(g, r, n, p, n, early, volt_ref, coef_ref, wave_ref)
                    for unit, q in todo[n * units + r * pairs + p]:
                        turn_pair(q, unit, plans[unit], wide_ref, coef_ref)
        final = pick(0, span)
        chosen = jnp.where(lax.broadcasted_iota(jnp.int32, final.shape, 1) < span, final, chosen)
        real = chosen[:subbands] * cos_late - chosen[subbands:] * sin_late
        imag = chosen[subbands:] * cos_late + chosen[:subbands] * sin_late
        for c in range(nchan):
            part = slice(c * block, (c + 1) * block)
            send_ref[c] = jnp.concatenate([real[part], imag[part]], axis=0).astype(jnp.bfloat16)

        pl.semaphore_wait(barrier, count - 1)

        def send(other, c):
            pltpu.make_async_remote_copy(
                src_ref=send_ref.at[c],
                dst_ref=recv_ref.at[me],
                send_sem=send_sem,
                recv_sem=recv_sem.at[my_set],
                device_id=other,
                device_id_type=LOGICAL,
            ).start()

        each_partner(send)
        recv_ref[me] = send_ref[chan_at]

        lanes = chan // RADIX
        wave = [wave_ref[r] for r in range(2)]
        split_wave = [
            tuple(wave[r][:, a * lanes : (a + 1) * lanes].astype(jnp.float32) for r in range(2))
            for a in range(RADIX)
        ]
        classes = eight_points(split_wave)
        basis_copy.wait()
        powers = []
        for c in range(RADIX):
            mixed = jnp.concatenate(classes[c], axis=1).astype(jnp.bfloat16)
            spec = jnp.dot(mixed, basis_ref[c], preferred_element_type=jnp.float32)
            both = spec[:, :lanes] * spec[:, :lanes] + spec[:, lanes:] * spec[:, lanes:]
            totals = []
            for g in range(groups):
                tiles = [
                    both[(g * FRAMES + f) * ROWS : (g * FRAMES + f + 1) * ROWS] for f in range(FRAMES)
                ]
                totals.append(sum(tiles[1:], tiles[0]))
            powers.append(jnp.concatenate(totals, axis=0) * (1.0 / FRAMES))
        wide = lanes // RADIX
        at = lax.broadcasted_iota(jnp.int32, (elems, lanes), 1)
        mixed = []
        for e in range(RADIX):
            piece = None
            for c in range(RADIX):
                shift = (wide * (c - e)) % lanes
                moved = pltpu.roll(powers[c], shift, 1) if shift else powers[c]
                piece = moved if piece is None else jnp.where(at // wide == c, moved, piece)
            mixed.append(piece)
        mixed = jnp.concatenate(mixed, axis=0).astype(jnp.bfloat16)
        down = lax.broadcasted_iota(jnp.int32, (lanes, lanes), 0)
        over = lax.broadcasted_iota(jnp.int32, (lanes, lanes), 1)
        back = (over == (down % wide) * RADIX + down // wide).astype(jnp.float32)
        final = jnp.dot(mixed, back.astype(jnp.bfloat16), preferred_element_type=jnp.float32)
        for e in range(RADIX):
            power_ref[:, e * lanes : (e + 1) * lanes] = final[e * elems : (e + 1) * elems].astype(
                jnp.bfloat16
            )

        down = lax.broadcasted_iota(jnp.int32, (weight_rows, block * wide_beams), 0)
        over = lax.broadcasted_iota(jnp.int32, (weight_rows, block * wide_beams), 1)
        target = down % block * wide_beams + down // block % 2 * (wide_beams // 2)
        sort = (over == target + down // (2 * block)).astype(jnp.float32).astype(jnp.bfloat16)
        weight_copy.wait()
        step = min(8, beams)
        for i in range(0, beams, step):
            piece = raw_ref[i : i + step].reshape(step * 2 * block, raw_ref.shape[3])
            weight_ref[2 * block * i : 2 * block * (i + step)] = piece

        def turn_weights(q, carry):
            depth = min(total, 8 * LANES)
            where = pl.multiple_of(q * depth, depth)
            turned = lax.dot_general(
                weight_ref[:, pl.ds(where, depth)], sort, TN, preferred_element_type=jnp.float32
            )
            for z in range(0, depth, LANES):
                tiles = [
                    turned[z + (i * groups + g) * ROWS : z + (i * groups + g + 1) * ROWS]
                    for g in range(groups)
                    for i in range(fan)
                ]
                turned_ref[pl.ds(pl.multiple_of(where + z, LANES), LANES), :] = jnp.concatenate(
                    tiles, axis=0
                ).astype(jnp.bfloat16)
            return carry

        if total <= 8 * LANES:
            turn_weights(0, 0)
        else:
            lax.fori_loop(0, total // (8 * LANES), turn_weights, 0)

    pl.run_scoped(
        front, pltpu.SemaphoreType.DMA((5,)), pltpu.SemaphoreType.DMA((groups + parts - 1,))
    )

    sets = count // gather
    place_at = lax.broadcasted_iota(jnp.int32, (2 * block, LANES), 1) // ROWS % fan
    low_row = lax.broadcasted_iota(jnp.int32, (2 * block, wide_beams), 0)

    def take(k, carry):
        which = jnp.where(near_start, k, sets - 1 - k)
        first = which * gather

        def arrived(n):
            some = recv_ref.at[pl.ds(0, n)]
            pltpu.make_async_copy(some, some, recv_sem.at[which]).wait()

        pl.when(which == my_set)(lambda: arrived(gather - 1))
        pl.when(which != my_set)(lambda: arrived(gather))
        pieces = [[] for _ in range(FRAMES)]
        for q in range(gather // fan):
            tiles = [recv_ref[first + q * fan + i].astype(jnp.float32) for i in range(fan)]
            for f in range(FRAMES):
                piece = None
                for i in range(fan):
                    shift = (ROWS * (i - f)) % LANES
                    moved = pltpu.roll(tiles[i], shift, 1) if shift else tiles[i]
                    piece = moved if piece is None else jnp.where(place_at == i, moved, piece)
                pieces[f].append(piece)
        picked = jnp.concatenate(
            [jnp.concatenate(p, axis=1) for p in pieces], axis=0
        ).astype(jnp.bfloat16)
        depth = gather * elems
        where = pl.multiple_of(which * depth, depth)
        product = jnp.dot(
            picked, turned_ref[pl.ds(where, depth), :], preferred_element_type=jnp.float32
        )
        out = []
        for f in range(FRAMES):
            tile = product[2 * block * f : 2 * block * (f + 1)]
            piece = tile[:, :wide_beams]
            for s in range(1, block):
                piece = jnp.where(
                    low_row % block == s, tile[:, s * wide_beams : (s + 1) * wide_beams], piece
                )
            out.append(piece if carry is None else carry[f] + piece)
        return tuple(out)

    if sets <= 8:
        sums = None
        for k in range(sets):
            sums = take(k, sums)
    else:
        zero = jnp.zeros((2 * block, wide_beams), jnp.float32)
        sums = lax.fori_loop(0, sets, take, (zero,) * FRAMES)
    for f in range(FRAMES):
        other = pltpu.roll(pltpu.roll(sums[f], wide_beams // 2, 1), block, 0)
        out = sums[f] + jnp.where(low_row < block, -other, other)
        for p in range(2):
            for s in range(block):
                at = p * block + s
                beam_ref[p, pl.ds(s * FRAMES + f, 1), :] = out[at : at + 1, :beams]

    sent = recv_ref.at[pl.ds(0, count - 1)]
    pltpu.make_async_copy(sent, sent, send_sem).wait()


def class_basis(chan):
    lanes = chan // RADIX
    b = np.arange(lanes)[:, None]
    d = np.arange(lanes)[None, :]
    out = []
    for c in range(RADIX):
        angle = 2.0 * np.pi / chan * (b * (c + RADIX * d) % chan)
        cos, sin = np.cos(angle) * chan**-0.5, np.sin(angle) * chan**-0.5
        out.append(np.block([[cos, -sin], [sin, cos]]))
    return jnp.asarray(np.stack(out), jnp.bfloat16)


def deliver_kernel(power_from, beam_from, power_to, beam_to, sems):
    copies = [
        pltpu.make_async_copy(power_from, power_to, sems.at[0]),
        pltpu.make_async_copy(beam_from, beam_to, sems.at[1]),
    ]
    for copy in copies:
        copy.start()
    for copy in copies:
        copy.wait()


def on_device(nelem, nchan, voltages, delays, prototype, subband_map, beam_weights):
    parts, elems, samples = voltages.shape
    taps, chan = prototype.shape
    beams, _, block, total = beam_weights.shape
    basis = class_basis(chan)
    count = nelem * nchan
    gather = 8
    wide_beams = max(LANES, 2 * beams)
    out_shape = [
        jax.ShapeDtypeStruct((elems, chan), jnp.bfloat16),
        jax.ShapeDtypeStruct((2, block * FRAMES, beams), jnp.float32),
    ]
    power, beam = pl.pallas_call(
        functools.partial(main_kernel, nelem, nchan, gather),
        in_specs=[pl.BlockSpec(memory_space=pltpu.HBM)] * 6,
        out_specs=[pl.BlockSpec(memory_space=pltpu.VMEM)] * 2,
        out_shape=[pltpu.VMEM(o.shape, o.dtype) for o in out_shape],
        scratch_shapes=[
            pltpu.SMEM(delays.shape, jnp.int32),
            pltpu.SMEM(subband_map.shape, jnp.int32),
            pltpu.VMEM((elems // ROWS, parts, ROWS, samples), jnp.bfloat16),
            pltpu.VMEM((taps, chan), jnp.bfloat16),
            pltpu.VMEM(beam_weights.shape, jnp.bfloat16),
            pltpu.VMEM(basis.shape, jnp.bfloat16),
            pltpu.VMEM((taps, chan), jnp.float32),
            pltpu.VMEM((elems // ROWS, taps, ROWS, chan), jnp.bfloat16),
            pltpu.VMEM((2, 2 * subband_map.shape[0], chan), jnp.bfloat16),
            pltpu.VMEM((parts, FRAMES * elems, chan), jnp.bfloat16),
            pltpu.VMEM((beams * 2 * block, total), jnp.bfloat16),
            pltpu.VMEM((total, block * wide_beams), jnp.bfloat16),
            pltpu.VMEM((nchan, 2 * block, FRAMES * elems), jnp.bfloat16),
            pltpu.VMEM((count, 2 * block, FRAMES * elems), jnp.bfloat16),
            pltpu.SemaphoreType.DMA,
            pltpu.SemaphoreType.DMA((count // gather,)),
        ],
        compiler_params=pltpu.CompilerParams(
            collective_id=0, has_side_effects=True, vmem_limit_bytes=66_400_000
        ),
    )(delays, subband_map, voltages, prototype, beam_weights, basis)
    return pl.pallas_call(
        deliver_kernel,
        in_specs=[pl.BlockSpec(memory_space=pl.ANY)] * 2,
        out_specs=[pl.BlockSpec(memory_space=pl.ANY)] * 2,
        out_shape=out_shape,
        scratch_shapes=[pltpu.SemaphoreType.DMA((2,))],
        compiler_params=pltpu.CompilerParams(vmem_limit_bytes=2**20),
    )(power, beam)


def solution(mesh):
    return jax.shard_map(
        functools.partial(on_device, mesh.shape["elem"], mesh.shape["chan"]),
        mesh=mesh,
        in_specs=(
            P(None, ("elem", "chan"), None),
            P(("elem", "chan")),
            P(),
            P(),
            P("elem", None, "chan", None),
        ),
        out_specs=(P(("elem", "chan"), None), P(None, "chan", "elem")),
        check_vma=False,
    )
```

```python
import functools
import math

import jax
import jax.numpy as jnp
import numpy as np
from jax import lax
from jax.experimental import pallas as pl
from jax.experimental.pallas import tpu as pltpu
from jax.sharding import PartitionSpec as P

FRAMES = 4
LANES = 128
ROWS = 8
RADIX = 8
LOGICAL = pl.DeviceIdType.LOGICAL
NT = (((1,), (1,)), ((), ()))
TN = (((0,), (0,)), ((), ()))


def cosine(turns, chan):
    y = jnp.abs((turns & (chan - 1)) - chan // 2) - chan // 4
    x = y.astype(jnp.float32) * (2.0 * math.pi / chan)
    s = x * x
    poly = 1.0 / 362880 - s * (1.0 / 39916800)
    poly = -1.0 / 5040 + s * poly
    poly = 1.0 / 120 + s * poly
    poly = -1.0 / 6 + s * poly
    return x + x * s * poly


def sine(turns, chan):
    return cosine(turns + 3 * (chan // 4), chan)


def eight_points(x):
    def add(a, b):
        return (a[0] + b[0], a[1] + b[1])

    def sub(a, b):
        return (a[0] - b[0], a[1] - b[1])

    def minus_i(a):
        return (a[1], -a[0])

    def four(v):
        a, b = add(v[0], v[2]), sub(v[0], v[2])
        c, d = add(v[1], v[3]), minus_i(sub(v[1], v[3]))
        return [add(a, c), add(b, d), sub(a, c), sub(b, d)]

    root = math.sqrt(0.5)
    even = four([add(x[a], x[a + 4]) for a in range(4)])
    d = [sub(x[a], x[a + 4]) for a in range(4)]
    d1 = ((d[1][0] + d[1][1]) * root, (d[1][1] - d[1][0]) * root)
    d3 = ((d[3][1] - d[3][0]) * root, (-d[3][0] - d[3][1]) * root)
    odd = four([d[0], d1, minus_i(d[2]), d3])
    out = []
    for e, o in zip(even, odd):
        out += [e, o]
    return out


def turn_plan(group, delay_ref):
    lane = lax.broadcasted_iota(jnp.int32, (ROWS, LANES), 1)
    sub = lax.broadcasted_iota(jnp.int32, (ROWS, LANES), 0)
    shift = jnp.zeros((ROWS, LANES), jnp.int32)
    for i in range(ROWS):
        shift = jnp.where(sub == i, delay_ref[group * ROWS + i], shift)
    return (lane - shift) & (LANES - 1), lane < LANES - shift, lane < shift


def turn_pair(pair, slot, plan, proto_ref, coef_ref):
    index, stay, _ = plan
    taps, chan = proto_ref.shape
    per = chan // LANES
    for t in range(taps):
        near = [
            jnp.broadcast_to(
                proto_ref[pl.ds(t, 1), pl.ds((2 * pair + i) % per * LANES, LANES)], (ROWS, LANES)
            )
            for i in (-1, 0, 1)
        ]
        turned = [
            jnp.take_along_axis(
                jnp.where(stay, near[i + 1], near[i]), index, axis=1, mode="promise_in_bounds"
            )
            for i in range(2)
        ]
        coef_ref[slot, t, :, pl.ds(2 * pair * LANES, 2 * LANES)] = jnp.concatenate(
            turned, axis=1
        ).astype(jnp.bfloat16)


def filter_pair(group, part, chunk, pair, slot, early, volt_ref, coef_ref, wave_ref):
    _, taps, _, chan = coef_ref.shape
    blocks = FRAMES + taps - 1
    wide = 2 * LANES

    def column(b, size):
        return volt_ref[chunk, part, :, pl.ds(b * chan + pair * wide, size)]

    held = [column(b, wide) for b in range(blocks)]
    if pair == 0:
        last = jnp.concatenate([column(blocks, LANES), held[-1][:, LANES:]], axis=1)
        held = [
            jnp.where(early, nxt, now) for now, nxt in zip(held, [*held[1:], last])
        ]
    stacks = [[] for _ in range(FRAMES)]
    for t in range(taps):
        coef = coef_ref[slot, t, :, pl.ds(pair * wide, wide)]
        for f in range(FRAMES):
            level, term = 0, coef * held[f + t]
            while stacks[f] and stacks[f][-1][0] == level:
                level, term = level + 1, stacks[f].pop()[1] + term
            stacks[f].append((level, term))
    for f in range(FRAMES):
        total = stacks[f].pop()[1]
        while stacks[f]:
            total = stacks[f].pop()[1] + total
        where = pl.ds((group * FRAMES + f) * ROWS, ROWS)
        wave_ref[part, where, pl.ds(pair * wide, wide)] = total


def main_kernel(
    nelem,
    nchan,
    gather,
    delay_hbm,
    map_hbm,
    volt_hbm,
    proto_hbm,
    weight_hbm,
    basis_hbm,
    power_ref,
    beam_ref,
    delay_ref,
    map_ref,
    volt_ref,
    proto_ref,
    raw_ref,
    basis_ref,
    wide_ref,
    coef_ref,
    pick_ref,
    wave_ref,
    weight_ref,
    turned_ref,
    send_ref,
    recv_ref,
    send_sem,
    recv_sem,
):
    parts, wave_rows, chan = wave_ref.shape
    groups = volt_ref.shape[0]
    elems = groups * ROWS
    taps = proto_ref.shape[0]
    per = chan // LANES
    count = nelem * nchan
    elem_at, chan_at = lax.axis_index("elem"), lax.axis_index("chan")
    me = elem_at * nchan + chan_at
    near_start = elem_at < nelem // 2
    barrier = pltpu.get_barrier_semaphore()

    def each_partner(act):
        def row(k, carry):
            first = jnp.where(near_start, nelem - 1 - k, k) * nchan
            for c in range(nchan):

                @pl.when(first + c != me)
                def _():
                    act(first + c, c)

            return carry

        if count <= 64:
            for k in range(nelem):
                row(k, 0)
        else:
            lax.fori_loop(0, nelem, row, 0)

    subbands = map_ref.shape[0]
    block = subbands // nchan
    my_set = me // gather
    beams = raw_ref.shape[0]
    weight_rows, total = weight_ref.shape
    wide_beams = turned_ref.shape[1] // block
    fan = LANES // elems

    def front(local_sem, volt_sem):
        order = [*range(1, groups), 0]
        map_copy = pltpu.make_async_copy(map_hbm, map_ref, local_sem.at[0])
        proto_copy = pltpu.make_async_copy(proto_hbm, proto_ref, local_sem.at[1])
        delay_copy = pltpu.make_async_copy(delay_hbm, delay_ref, local_sem.at[2])
        basis_copy = pltpu.make_async_copy(basis_hbm, basis_ref, local_sem.at[3])
        weight_copy = pltpu.make_async_copy(weight_hbm, raw_ref, local_sem.at[4])
        volt_copies = [
            pltpu.make_async_copy(
                volt_hbm.at[r, pl.ds(order[0] * ROWS, ROWS)], volt_ref.at[0, r], volt_sem.at[r]
            )
            for r in range(parts)
        ]
        for k, g in enumerate(order[1:]):
            volt_copies.append(
                pltpu.make_async_copy(
                    volt_hbm.at[:, pl.ds(g * ROWS, ROWS)],
                    volt_ref.at[k + 1],
                    volt_sem.at[k + parts],
                )
            )
        proto_copy.start()
        delay_copy.start()
        map_copy.start()
        for copy in volt_copies[: parts + 1]:
            copy.start()

        def greet(other, c):
            pl.semaphore_signal(barrier, inc=1, device_id=other, device_id_type=LOGICAL)

        each_partner(greet)
        for copy in volt_copies[parts + 1 :]:
            copy.start()

        map_copy.wait()
        delay_copy.wait()
        proto_copy.wait()
        wide_ref[...] = proto_ref[...].astype(jnp.float32)
        still = jnp.where(me < 0, 1, 0)
        pairs = per // 2
        plans = [turn_plan(g, delay_ref) for g in order]
        turn_pair(0, 0, plans[0], wide_ref, coef_ref)
        row = lax.broadcasted_iota(jnp.int32, (subbands, LANES), 0)
        lane = lax.broadcasted_iota(jnp.int32, (subbands, LANES), 1)
        wanted = jnp.zeros((subbands, LANES), jnp.int32)
        for s in range(subbands):
            wanted = jnp.where(row == s, map_ref[s], wanted)
        scale = chan**-0.5
        cos, sin = cosine(wanted * lane, chan) * scale, sine(wanted * lane, chan) * scale
        cos_step, sin_step = cosine(wanted * LANES, chan), sine(wanted * LANES, chan)
        for j in range(per):
            if j:
                cos, sin = cos * cos_step - sin * sin_step, sin * cos_step + cos * sin_step
            where = pl.ds(j * LANES, LANES)
            pick_ref[0, pl.ds(0, subbands), where] = cos.astype(jnp.bfloat16)
            pick_ref[0, pl.ds(subbands, subbands), where] = (-sin).astype(jnp.bfloat16)
            pick_ref[1, pl.ds(0, subbands), where] = sin.astype(jnp.bfloat16)
            pick_ref[1, pl.ds(subbands, subbands), where] = cos.astype(jnp.bfloat16)
        column = lax.broadcasted_iota(jnp.int32, (ROWS, LANES), 1)
        column = column // (FRAMES * ROWS) * ROWS + column % ROWS
        late = jnp.zeros((ROWS, LANES), jnp.int32)
        for e in range(elems):
            late = jnp.where(column == e, delay_ref[e], late)
        late = jnp.concatenate([late] * (subbands // ROWS), axis=0)
        cos_late, sin_late = cosine(wanted * late, chan), sine(wanted * late, chan)

        span = FRAMES * ROWS

        def pick(first, size):
            both = sum(
                lax.dot_general(
                    pick_ref[r],
                    wave_ref[r, pl.ds(first, size)],
                    NT,
                    preferred_element_type=jnp.float32,
                )
                for r in range(parts)
            )
            both = [both]
            if first:
                both = [jnp.zeros((2 * subbands, first), jnp.float32), *both]
            if first + size < LANES:
                both.append(jnp.zeros((2 * subbands, LANES - first - size), jnp.float32))
            return jnp.concatenate(both, axis=1)

        units = parts * pairs
        todo = [[] for _ in range(groups * units)]
        for p in range(1, pairs):
            todo[p - 1].append((0, p))
        later = [(n, p) for n in range(1, groups) for p in range(pairs)]
        ahead = [[] for _ in range(groups * units)]
        ahead[pairs - 1], later = later[: pairs - 1], later[pairs - 1 :]
        ahead[2 * pairs - 1], later = later[:1], later[1:]
        ahead[units + parts * pairs - 1] = later
        for n, g in enumerate(order):
            if n < groups - 1:
                volt_copies[n + parts - 1 if n else 0].wait()
            if n == groups - 2:
                basis_copy.start()
                weight_copy.start()
            early = plans[n][2].astype(jnp.int32)
            early = jnp.concatenate([early, jnp.zeros_like(early)], axis=1) != 0
            for r in range(parts):
                if n == 0 and r:
                    volt_copies[r].wait()
                if n == groups - 2 and r == parts - 1:
                    volt_copies[-1].wait()
                if n == groups - 2 and r == parts - 1:
                    chosen = pick(span, n * span)
                if n == groups - 1 and r == 0:
                    chosen = chosen + pick(n * span, span)
                for p in range(pairs):
                    for unit, q in ahead[n * units + r * pairs + p]:
                        turn_pair(q, unit + still, plans[unit], wide_ref, coef_ref)
                    filter_pair(g, r, n, p, n, early, volt_ref, coef_ref, wave_ref)
                    for unit, q in todo[n * units + r * pairs + p]:
                        turn_pair(q, unit, plans[unit], wide_ref, coef_ref)
        final = pick(0, span)
        chosen = jnp.where(lax.broadcasted_iota(jnp.int32, final.shape, 1) < span, final, chosen)
        real = chosen[:subbands] * cos_late - chosen[subbands:] * sin_late
        imag = chosen[subbands:] * cos_late + chosen[:subbands] * sin_late
        for c in range(nchan):
            part = slice(c * block, (c + 1) * block)
            send_ref[c] = jnp.concatenate([real[part], imag[part]], axis=0).astype(jnp.bfloat16)

        pl.semaphore_wait(barrier, count - 1)

        def send(other, c):
            pltpu.make_async_remote_copy(
                src_ref=send_ref.at[c],
                dst_ref=recv_ref.at[me],
                send_sem=send_sem,
                recv_sem=recv_sem.at[my_set],
                device_id=other,
                device_id_type=LOGICAL,
            ).start()

        each_partner(send)
        recv_ref[me] = send_ref[chan_at]

        lanes = chan // RADIX
        wave = [wave_ref[r] for r in range(2)]
        split_wave = [
            tuple(wave[r][:, a * lanes : (a + 1) * lanes].astype(jnp.float32) for r in range(2))
            for a in range(RADIX)
        ]
        classes = eight_points(split_wave)
        basis_copy.wait()
        powers = []
        for c in range(RADIX):
            mixed = jnp.concatenate(classes[c], axis=1).astype(jnp.bfloat16)
            spec = jnp.dot(mixed, basis_ref[c], preferred_element_type=jnp.float32)
            both = spec[:, :lanes] * spec[:, :lanes] + spec[:, lanes:] * spec[:, lanes:]
            totals = []
            for g in range(groups):
                tiles = [
                    both[(g * FRAMES + f) * ROWS : (g * FRAMES + f + 1) * ROWS] for f in range(FRAMES)
                ]
                totals.append(sum(tiles[1:], tiles[0]))
            powers.append(jnp.concatenate(totals, axis=0) * (1.0 / FRAMES))
        wide = lanes // RADIX
        at = lax.broadcasted_iota(jnp.int32, (elems, lanes), 1)
        mixed = []
        for e in range(RADIX):
            piece = None
            for c in range(RADIX):
                shift = (wide * (c - e)) % lanes
                moved = pltpu.roll(powers[c], shift, 1) if shift else powers[c]
                piece = moved if piece is None else jnp.where(at // wide == c, moved, piece)
            mixed.append(piece)
        mixed = jnp.concatenate(mixed, axis=0).astype(jnp.bfloat16)
        down = lax.broadcasted_iota(jnp.int32, (lanes, lanes), 0)
        over = lax.broadcasted_iota(jnp.int32, (lanes, lanes), 1)
        back = (over == (down % wide) * RADIX + down // wide).astype(jnp.float32)
        final = jnp.dot(mixed, back.astype(jnp.bfloat16), preferred_element_type=jnp.float32)
        for e in range(RADIX):
            power_ref[:, e * lanes : (e + 1) * lanes] = final[e * elems : (e + 1) * elems].astype(
                jnp.bfloat16
            )

        down = lax.broadcasted_iota(jnp.int32, (weight_rows, block * wide_beams), 0)
        over = lax.broadcasted_iota(jnp.int32, (weight_rows, block * wide_beams), 1)
        target = down % block * wide_beams + down // block % 2 * (wide_beams // 2)
        sort = (over == target + down // (2 * block)).astype(jnp.float32).astype(jnp.bfloat16)
        weight_copy.wait()
        step = min(8, beams)
        for i in range(0, beams, step):
            piece = raw_ref[i : i + step].reshape(step * 2 * block, raw_ref.shape[3])
            weight_ref[2 * block * i : 2 * block * (i + step)] = piece

        def turn_weights(q, carry):
            depth = min(total, 8 * LANES)
            where = pl.multiple_of(q * depth, depth)
            turned = lax.dot_general(
                weight_ref[:, pl.ds(where, depth)], sort, TN, preferred_element_type=jnp.float32
            )
            for z in range(0, depth, LANES):
                tiles = [
                    turned[z + (i * groups + g) * ROWS : z + (i * groups + g + 1) * ROWS]
                    for g in range(groups)
                    for i in range(fan)
                ]
                turned_ref[pl.ds(pl.multiple_of(where + z, LANES), LANES), :] = jnp.concatenate(
                    tiles, axis=0
                ).astype(jnp.bfloat16)
            return carry

        if total <= 8 * LANES:
            turn_weights(0, 0)
        else:
            lax.fori_loop(0, total // (8 * LANES), turn_weights, 0)

    pl.run_scoped(
        front, pltpu.SemaphoreType.DMA((5,)), pltpu.SemaphoreType.DMA((groups + parts - 1,))
    )

    sets = count // gather
    place_at = lax.broadcasted_iota(jnp.int32, (2 * block, LANES), 1) // ROWS % fan
    low_row = lax.broadcasted_iota(jnp.int32, (2 * block, wide_beams), 0)

    def take(k, carry):
        which = jnp.where(near_start, k, sets - 1 - k)
        first = which * gather

        def arrived(n):
            some = recv_ref.at[pl.ds(0, n)]
            pltpu.make_async_copy(some, some, recv_sem.at[which]).wait()

        pl.when(which == my_set)(lambda: arrived(gather - 1))
        pl.when(which != my_set)(lambda: arrived(gather))
        pieces = [[] for _ in range(FRAMES)]
        for q in range(gather // fan):
            tiles = [recv_ref[first + q * fan + i].astype(jnp.float32) for i in range(fan)]
            for f in range(FRAMES):
                piece = None
                for i in range(fan):
                    shift = (ROWS * (i - f)) % LANES
                    moved = pltpu.roll(tiles[i], shift, 1) if shift else tiles[i]
                    piece = moved if piece is None else jnp.where(place_at == i, moved, piece)
                pieces[f].append(piece)
        picked = jnp.concatenate(
            [jnp.concatenate(p, axis=1) for p in pieces], axis=0
        ).astype(jnp.bfloat16)
        depth = gather * elems
        where = pl.multiple_of(which * depth, depth)
        product = jnp.dot(
            picked, turned_ref[pl.ds(where, depth), :], preferred_element_type=jnp.float32
        )
        out = []
        for f in range(FRAMES):
            tile = product[2 * block * f : 2 * block * (f + 1)]
            piece = tile[:, :wide_beams]
            for s in range(1, block):
                piece = jnp.where(
                    low_row % block == s, tile[:, s * wide_beams : (s + 1) * wide_beams], piece
                )
            out.append(piece if carry is None else carry[f] + piece)
        return tuple(out)

    if sets <= 8:
        sums = None
        for k in range(sets):
            sums = take(k, sums)
    else:
        zero = jnp.zeros((2 * block, wide_beams), jnp.float32)
        sums = lax.fori_loop(0, sets, take, (zero,) * FRAMES)
    for f in range(FRAMES):
        other = pltpu.roll(pltpu.roll(sums[f], wide_beams // 2, 1), block, 0)
        out = sums[f] + jnp.where(low_row < block, -other, other)
        for p in range(2):
            for s in range(block):
                at = p * block + s
                beam_ref[p, pl.ds(s * FRAMES + f, 1), :] = out[at : at + 1, :beams]

    sent = recv_ref.at[pl.ds(0, count - 1)]
    pltpu.make_async_copy(sent, sent, send_sem).wait()


def class_basis(chan):
    lanes = chan // RADIX
    b = np.arange(lanes)[:, None]
    d = np.arange(lanes)[None, :]
    out = []
    for c in range(RADIX):
        angle = 2.0 * np.pi / chan * (b * (c + RADIX * d) % chan)
        cos, sin = np.cos(angle) * chan**-0.5, np.sin(angle) * chan**-0.5
        out.append(np.block([[cos, -sin], [sin, cos]]))
    return jnp.asarray(np.stack(out), jnp.bfloat16)


def deliver_kernel(power_from, beam_from, power_to, beam_to):
    def deliver(sems):
        copies = [
            pltpu.make_async_copy(power_from, power_to, sems.at[0]),
            pltpu.make_async_copy(beam_from, beam_to, sems.at[1]),
        ]
        for copy in copies:
            copy.start()
        for copy in copies:
            copy.wait()

    pl.run_scoped(deliver, pltpu.SemaphoreType.DMA((2,)))


def on_device(nelem, nchan, voltages, delays, prototype, subband_map, beam_weights):
    parts, elems, samples = voltages.shape
    taps, chan = prototype.shape
    beams, _, block, total = beam_weights.shape
    basis = class_basis(chan)
    count = nelem * nchan
    gather = 8
    wide_beams = max(LANES, 2 * beams)
    out_shape = [
        jax.ShapeDtypeStruct((elems, chan), jnp.bfloat16),
        jax.ShapeDtypeStruct((2, block * FRAMES, beams), jnp.float32),
    ]
    power, beam = pl.pallas_call(
        functools.partial(main_kernel, nelem, nchan, gather),
        in_specs=[pl.BlockSpec(memory_space=pltpu.HBM)] * 6,
        out_specs=[pl.BlockSpec(memory_space=pltpu.VMEM)] * 2,
        out_shape=[pltpu.VMEM(o.shape, o.dtype) for o in out_shape],
        scratch_shapes=[
            pltpu.SMEM(delays.shape, jnp.int32),
            pltpu.SMEM(subband_map.shape, jnp.int32),
            pltpu.VMEM((elems // ROWS, parts, ROWS, samples), jnp.bfloat16),
            pltpu.VMEM((taps, chan), jnp.bfloat16),
            pltpu.VMEM(beam_weights.shape, jnp.bfloat16),
            pltpu.VMEM(basis.shape, jnp.bfloat16),
            pltpu.VMEM((taps, chan), jnp.float32),
            pltpu.VMEM((elems // ROWS, taps, ROWS, chan), jnp.bfloat16),
            pltpu.VMEM((2, 2 * subband_map.shape[0], chan), jnp.bfloat16),
            pltpu.VMEM((parts, FRAMES * elems, chan), jnp.bfloat16),
            pltpu.VMEM((beams * 2 * block, total), jnp.bfloat16),
            pltpu.VMEM((total, block * wide_beams), jnp.bfloat16),
            pltpu.VMEM((nchan, 2 * block, FRAMES * elems), jnp.bfloat16),
            pltpu.VMEM((count, 2 * block, FRAMES * elems), jnp.bfloat16),
            pltpu.SemaphoreType.DMA,
            pltpu.SemaphoreType.DMA((count // gather,)),
        ],
        compiler_params=pltpu.CompilerParams(
            collective_id=0, has_side_effects=True, vmem_limit_bytes=66_400_000
        ),
    )(delays, subband_map, voltages, prototype, beam_weights, basis)
    return pl.pallas_call(
        deliver_kernel,
        in_specs=[pl.BlockSpec(memory_space=pl.ANY)] * 2,
        out_specs=[pl.BlockSpec(memory_space=pl.ANY)] * 2,
        out_shape=out_shape,
        compiler_params=pltpu.CompilerParams(vmem_limit_bytes=2**20),
    )(power, beam)


def solution(mesh):
    return jax.shard_map(
        functools.partial(on_device, mesh.shape["elem"], mesh.shape["chan"]),
        mesh=mesh,
        in_specs=(
            P(None, ("elem", "chan"), None),
            P(("elem", "chan")),
            P(),
            P(),
            P("elem", None, "chan", None),
        ),
        out_specs=(P(("elem", "chan"), None), P(None, "chan", "elem")),
        check_vma=False,
    )
```

```python
import functools
import math

import jax
import jax.numpy as jnp
import numpy as np
from jax import lax
from jax.experimental import pallas as pl
from jax.experimental.pallas import tpu as pltpu
from jax.sharding import PartitionSpec as P

FRAMES = 4
LANES = 128
ROWS = 8
RADIX = 8
LOGICAL = pl.DeviceIdType.LOGICAL
NT = (((1,), (1,)), ((), ()))
TN = (((0,), (0,)), ((), ()))


def cosine(turns, chan):
    y = jnp.abs((turns & (chan - 1)) - chan // 2) - chan // 4
    x = y.astype(jnp.float32) * (2.0 * math.pi / chan)
    s = x * x
    poly = 1.0 / 362880 - s * (1.0 / 39916800)
    poly = -1.0 / 5040 + s * poly
    poly = 1.0 / 120 + s * poly
    poly = -1.0 / 6 + s * poly
    return x + x * s * poly


def sine(turns, chan):
    return cosine(turns + 3 * (chan // 4), chan)


def eight_points(x):
    def add(a, b):
        return (a[0] + b[0], a[1] + b[1])

    def sub(a, b):
        return (a[0] - b[0], a[1] - b[1])

    def minus_i(a):
        return (a[1], -a[0])

    def four(v):
        a, b = add(v[0], v[2]), sub(v[0], v[2])
        c, d = add(v[1], v[3]), minus_i(sub(v[1], v[3]))
        return [add(a, c), add(b, d), sub(a, c), sub(b, d)]

    root = math.sqrt(0.5)
    even = four([add(x[a], x[a + 4]) for a in range(4)])
    d = [sub(x[a], x[a + 4]) for a in range(4)]
    d1 = ((d[1][0] + d[1][1]) * root, (d[1][1] - d[1][0]) * root)
    d3 = ((d[3][1] - d[3][0]) * root, (-d[3][0] - d[3][1]) * root)
    odd = four([d[0], d1, minus_i(d[2]), d3])
    out = []
    for e, o in zip(even, odd):
        out += [e, o]
    return out


def turn_plan(group, delay_ref):
    lane = lax.broadcasted_iota(jnp.int32, (ROWS, LANES), 1)
    sub = lax.broadcasted_iota(jnp.int32, (ROWS, LANES), 0)
    shift = jnp.zeros((ROWS, LANES), jnp.int32)
    for i in range(ROWS):
        shift = jnp.where(sub == i, delay_ref[group * ROWS + i], shift)
    return (lane - shift) & (LANES - 1), lane < LANES - shift, lane < shift


def turn_pair(pair, slot, plan, proto_ref, coef_ref):
    index, stay, _ = plan
    taps, chan = proto_ref.shape
    per = chan // LANES
    for t in range(taps):
        near = [
            jnp.broadcast_to(
                proto_ref[pl.ds(t, 1), pl.ds((2 * pair + i) % per * LANES, LANES)], (ROWS, LANES)
            )
            for i in (-1, 0, 1)
        ]
        turned = [
            jnp.take_along_axis(
                jnp.where(stay, near[i + 1], near[i]), index, axis=1, mode="promise_in_bounds"
            )
            for i in range(2)
        ]
        coef_ref[slot, t, :, pl.ds(2 * pair * LANES, 2 * LANES)] = jnp.concatenate(
            turned, axis=1
        ).astype(jnp.bfloat16)


def filter_pair(group, part, chunk, pair, slot, early, volt_ref, coef_ref, wave_ref):
    _, taps, _, chan = coef_ref.shape
    blocks = FRAMES + taps - 1
    wide = 2 * LANES

    def column(b, size):
        return volt_ref[chunk, part, :, pl.ds(b * chan + pair * wide, size)]

    held = [column(b, wide) for b in range(blocks)]
    if pair == 0:
        last = jnp.concatenate([column(blocks, LANES), held[-1][:, LANES:]], axis=1)
        held = [
            jnp.where(early, nxt, now) for now, nxt in zip(held, [*held[1:], last])
        ]
    stacks = [[] for _ in range(FRAMES)]
    for t in range(taps):
        coef = coef_ref[slot, t, :, pl.ds(pair * wide, wide)]
        for f in range(FRAMES):
            level, term = 0, coef * held[f + t]
            while stacks[f] and stacks[f][-1][0] == level:
                level, term = level + 1, stacks[f].pop()[1] + term
            stacks[f].append((level, term))
    for f in range(FRAMES):
        total = stacks[f].pop()[1]
        while stacks[f]:
            total = stacks[f].pop()[1] + total
        where = pl.ds((group * FRAMES + f) * ROWS, ROWS)
        wave_ref[part, where, pl.ds(pair * wide, wide)] = total


def main_kernel(
    nelem,
    nchan,
    gather,
    delay_hbm,
    map_hbm,
    volt_hbm,
    proto_hbm,
    weight_hbm,
    basis_hbm,
    power_ref,
    beam_ref,
    delay_ref,
    map_ref,
    volt_ref,
    proto_ref,
    raw_ref,
    basis_ref,
    wide_ref,
    coef_ref,
    pick_ref,
    wave_ref,
    weight_ref,
    turned_ref,
    swapped_ref,
    send_ref,
    recv_ref,
    send_sem,
    recv_sem,
):
    parts, wave_rows, chan = wave_ref.shape
    groups = volt_ref.shape[0]
    elems = groups * ROWS
    taps = proto_ref.shape[0]
    per = chan // LANES
    count = nelem * nchan
    elem_at, chan_at = lax.axis_index("elem"), lax.axis_index("chan")
    me = elem_at * nchan + chan_at
    near_start = elem_at < nelem // 2
    barrier = pltpu.get_barrier_semaphore()

    def each_partner(act):
        def row(k, carry):
            first = jnp.where(near_start, nelem - 1 - k, k) * nchan
            for c in range(nchan):

                @pl.when(first + c != me)
                def _():
                    act(first + c, c)

            return carry

        if count <= 64:
            for k in range(nelem):
                row(k, 0)
        else:
            lax.fori_loop(0, nelem, row, 0)

    subbands = map_ref.shape[0]
    block = subbands // nchan
    my_set = me // gather
    beams = raw_ref.shape[0]
    weight_rows, total = weight_ref.shape
    wide_beams = turned_ref.shape[1] // block
    fan = LANES // elems
    sets = count // gather
    depth = gather * elems
    few = sets <= 8

    def front(local_sem, volt_sem):
        order = [*range(1, groups), 0]
        map_copy = pltpu.make_async_copy(map_hbm, map_ref, local_sem.at[0])
        proto_copy = pltpu.make_async_copy(proto_hbm, proto_ref, local_sem.at[1])
        delay_copy = pltpu.make_async_copy(delay_hbm, delay_ref, local_sem.at[2])
        basis_copy = pltpu.make_async_copy(basis_hbm, basis_ref, local_sem.at[3])
        weight_copy = pltpu.make_async_copy(weight_hbm, raw_ref, local_sem.at[4])
        volt_copies = [
            pltpu.make_async_copy(
                volt_hbm.at[r, pl.ds(order[0] * ROWS, ROWS)], volt_ref.at[0, r], volt_sem.at[r]
            )
            for r in range(parts)
        ]
        for k, g in enumerate(order[1:]):
            volt_copies.append(
                pltpu.make_async_copy(
                    volt_hbm.at[:, pl.ds(g * ROWS, ROWS)],
                    volt_ref.at[k + 1],
                    volt_sem.at[k + parts],
                )
            )
        proto_copy.start()
        delay_copy.start()
        map_copy.start()
        for copy in volt_copies[: parts + 1]:
            copy.start()

        def greet(other, c):
            pl.semaphore_signal(barrier, inc=1, device_id=other, device_id_type=LOGICAL)

        each_partner(greet)
        for copy in volt_copies[parts + 1 :]:
            copy.start()

        map_copy.wait()
        delay_copy.wait()
        proto_copy.wait()
        wide_ref[...] = proto_ref[...].astype(jnp.float32)
        still = jnp.where(me < 0, 1, 0)
        pairs = per // 2
        plans = [turn_plan(g, delay_ref) for g in order]
        turn_pair(0, 0, plans[0], wide_ref, coef_ref)
        row = lax.broadcasted_iota(jnp.int32, (subbands, LANES), 0)
        lane = lax.broadcasted_iota(jnp.int32, (subbands, LANES), 1)
        wanted = jnp.zeros((subbands, LANES), jnp.int32)
        for s in range(subbands):
            wanted = jnp.where(row == s, map_ref[s], wanted)
        scale = chan**-0.5
        cos, sin = cosine(wanted * lane, chan) * scale, sine(wanted * lane, chan) * scale
        cos_step, sin_step = cosine(wanted * LANES, chan), sine(wanted * LANES, chan)
        for j in range(per):
            if j:
                cos, sin = cos * cos_step - sin * sin_step, sin * cos_step + cos * sin_step
            where = pl.ds(j * LANES, LANES)
            pick_ref[0, pl.ds(0, subbands), where] = cos.astype(jnp.bfloat16)
            pick_ref[0, pl.ds(subbands, subbands), where] = (-sin).astype(jnp.bfloat16)
            pick_ref[1, pl.ds(0, subbands), where] = sin.astype(jnp.bfloat16)
            pick_ref[1, pl.ds(subbands, subbands), where] = cos.astype(jnp.bfloat16)
        column = lax.broadcasted_iota(jnp.int32, (ROWS, LANES), 1)
        column = column // (FRAMES * ROWS) * ROWS + column % ROWS
        late = jnp.zeros((ROWS, LANES), jnp.int32)
        for e in range(elems):
            late = jnp.where(column == e, delay_ref[e], late)
        late = jnp.concatenate([late] * (subbands // ROWS), axis=0)
        cos_late, sin_late = cosine(wanted * late, chan), sine(wanted * late, chan)

        span = FRAMES * ROWS

        def pick(first, size):
            both = sum(
                lax.dot_general(
                    pick_ref[r],
                    wave_ref[r, pl.ds(first, size)],
                    NT,
                    preferred_element_type=jnp.float32,
                )
                for r in range(parts)
            )
            both = [both]
            if first:
                both = [jnp.zeros((2 * subbands, first), jnp.float32), *both]
            if first + size < LANES:
                both.append(jnp.zeros((2 * subbands, LANES - first - size), jnp.float32))
            return jnp.concatenate(both, axis=1)

        units = parts * pairs
        todo = [[] for _ in range(groups * units)]
        for p in range(1, pairs):
            todo[p - 1].append((0, p))
        later = [(n, p) for n in range(1, groups) for p in range(pairs)]
        ahead = [[] for _ in range(groups * units)]
        ahead[pairs - 1], later = later[: pairs - 1], later[pairs - 1 :]
        ahead[2 * pairs - 1], later = later[:1], later[1:]
        ahead[units + parts * pairs - 1] = later
        for n, g in enumerate(order):
            if n < groups - 1:
                volt_copies[n + parts - 1 if n else 0].wait()
            if n == groups - 2:
                basis_copy.start()
                weight_copy.start()
            early = plans[n][2].astype(jnp.int32)
            early = jnp.concatenate([early, jnp.zeros_like(early)], axis=1) != 0
            for r in range(parts):
                if n == 0 and r:
                    volt_copies[r].wait()
                if n == groups - 2 and r == parts - 1:
                    volt_copies[-1].wait()
                if n == groups - 2 and r == parts - 1:
                    chosen = pick(span, n * span)
                if n == groups - 1 and r == 0:
                    chosen = chosen + pick(n * span, span)
                for p in range(pairs):
                    for unit, q in ahead[n * units + r * pairs + p]:
                        turn_pair(q, unit + still, plans[unit], wide_ref, coef_ref)
                    filter_pair(g, r, n, p, n, early, volt_ref, coef_ref, wave_ref)
                    for unit, q in todo[n * units + r * pairs + p]:
                        turn_pair(q, unit, plans[unit], wide_ref, coef_ref)
        final = pick(0, span)
        chosen = jnp.where(lax.broadcasted_iota(jnp.int32, final.shape, 1) < span, final, chosen)
        real = chosen[:subbands] * cos_late - chosen[subbands:] * sin_late
        imag = chosen[subbands:] * cos_late + chosen[:subbands] * sin_late
        for c in range(nchan):
            part = slice(c * block, (c + 1) * block)
            send_ref[c] = jnp.concatenate([real[part], imag[part]], axis=0).astype(jnp.bfloat16)

        pl.semaphore_wait(barrier, count - 1)

        def send(other, c):
            pltpu.make_async_remote_copy(
                src_ref=send_ref.at[c],
                dst_ref=recv_ref.at[me],
                send_sem=send_sem,
                recv_sem=recv_sem.at[my_set],
                device_id=other,
                device_id_type=LOGICAL,
            ).start()

        each_partner(send)
        recv_ref[me] = send_ref[chan_at]

        lanes = chan // RADIX
        wave = [wave_ref[r] for r in range(2)]
        split_wave = [
            tuple(wave[r][:, a * lanes : (a + 1) * lanes].astype(jnp.float32) for r in range(2))
            for a in range(RADIX)
        ]
        classes = eight_points(split_wave)
        basis_copy.wait()
        powers = []
        for c in range(RADIX):
            mixed = jnp.concatenate(classes[c], axis=1).astype(jnp.bfloat16)
            spec = jnp.dot(mixed, basis_ref[c], preferred_element_type=jnp.float32)
            both = spec[:, :lanes] * spec[:, :lanes] + spec[:, lanes:] * spec[:, lanes:]
            totals = []
            for g in range(groups):
                tiles = [
                    both[(g * FRAMES + f) * ROWS : (g * FRAMES + f + 1) * ROWS] for f in range(FRAMES)
                ]
                totals.append(sum(tiles[1:], tiles[0]))
            powers.append(jnp.concatenate(totals, axis=0) * (1.0 / FRAMES))
        wide = lanes // RADIX
        at = lax.broadcasted_iota(jnp.int32, (elems, lanes), 1)
        mixed = []
        for e in range(RADIX):
            piece = None
            for c in range(RADIX):
                shift = (wide * (c - e)) % lanes
                moved = pltpu.roll(powers[c], shift, 1) if shift else powers[c]
                piece = moved if piece is None else jnp.where(at // wide == c, moved, piece)
            mixed.append(piece)
        mixed = jnp.concatenate(mixed, axis=0).astype(jnp.bfloat16)
        down = lax.broadcasted_iota(jnp.int32, (lanes, lanes), 0)
        over = lax.broadcasted_iota(jnp.int32, (lanes, lanes), 1)
        back = (over == (down % wide) * RADIX + down // wide).astype(jnp.float32)
        final = jnp.dot(mixed, back.astype(jnp.bfloat16), preferred_element_type=jnp.float32)
        for e in range(RADIX):
            power_ref[:, e * lanes : (e + 1) * lanes] = final[e * elems : (e + 1) * elems].astype(
                jnp.bfloat16
            )

        down = lax.broadcasted_iota(jnp.int32, (weight_rows, block * wide_beams), 0)
        over = lax.broadcasted_iota(jnp.int32, (weight_rows, block * wide_beams), 1)
        target = down % block * wide_beams + down // block % 2 * (wide_beams // 2)
        sort = (over == target + down // (2 * block)).astype(jnp.float32).astype(jnp.bfloat16)
        weight_copy.wait()
        step = min(8, beams)
        for i in range(0, beams, step):
            piece = raw_ref[i : i + step].reshape(step * 2 * block, raw_ref.shape[3])
            weight_ref[2 * block * i : 2 * block * (i + step)] = piece

        def turn_weights(q, carry):
            depth = min(total, 8 * LANES)
            where = pl.multiple_of(q * depth, depth)
            turned = lax.dot_general(
                weight_ref[:, pl.ds(where, depth)], sort, TN, preferred_element_type=jnp.float32
            )
            for z in range(0, depth, LANES):
                tiles = [
                    turned[z + (i * groups + g) * ROWS : z + (i * groups + g + 1) * ROWS]
                    for g in range(groups)
                    for i in range(fan)
                ]
                turned_ref[pl.ds(pl.multiple_of(where + z, LANES), LANES), :] = jnp.concatenate(
                    tiles, axis=0
                ).astype(jnp.bfloat16)
            return carry

        if total <= 8 * LANES:
            turn_weights(0, 0)
        else:
            lax.fori_loop(0, total // (8 * LANES), turn_weights, 0)
        if few:
            final_set = pl.multiple_of(jnp.where(near_start, sets - 1, 0) * depth, depth)
            for b in range(block):
                where = pl.ds(b * wide_beams, wide_beams)
                tile = turned_ref[pl.ds(final_set, depth), where].astype(jnp.float32)
                swapped_ref[:, where] = pltpu.roll(tile, wide_beams // 2, 1).astype(jnp.bfloat16)

    pl.run_scoped(
        front, pltpu.SemaphoreType.DMA((5,)), pltpu.SemaphoreType.DMA((groups + parts - 1,))
    )

    place_at = lax.broadcasted_iota(jnp.int32, (2 * block, LANES), 1) // ROWS % fan
    low_row = lax.broadcasted_iota(jnp.int32, (2 * block, wide_beams), 0)

    def take(k, carry, swap=None):
        before = swap_of(carry) if swap is not None else None
        which = jnp.where(near_start, k, sets - 1 - k)
        first = which * gather

        def arrived(n):
            some = recv_ref.at[pl.ds(0, n)]
            pltpu.make_async_copy(some, some, recv_sem.at[which]).wait()

        pl.when(which == my_set)(lambda: arrived(gather - 1))
        pl.when(which != my_set)(lambda: arrived(gather))
        pieces = [[] for _ in range(FRAMES)]
        for q in range(gather // fan):
            tiles = [recv_ref[first + q * fan + i].astype(jnp.float32) for i in range(fan)]
            for f in range(FRAMES):
                piece = None
                for i in range(fan):
                    shift = (ROWS * (i - f)) % LANES
                    moved = pltpu.roll(tiles[i], shift, 1) if shift else tiles[i]
                    piece = moved if piece is None else jnp.where(place_at == i, moved, piece)
                pieces[f].append(piece)
        picked = jnp.concatenate(
            [jnp.concatenate(p, axis=1) for p in pieces], axis=0
        ).astype(jnp.bfloat16)
        where = pl.multiple_of(which * depth, depth)

        def through(weights):
            product = jnp.dot(picked, weights, preferred_element_type=jnp.float32)
            out = []
            for f in range(FRAMES):
                tile = product[2 * block * f : 2 * block * (f + 1)]
                piece = tile[:, :wide_beams]
                for s in range(1, block):
                    own = tile[:, s * wide_beams : (s + 1) * wide_beams]
                    piece = jnp.where(low_row % block == s, own, piece)
                out.append(piece)
            return out

        out = through(turned_ref[pl.ds(where, depth), :])
        if swap is not None:
            swap += [s + o for s, o in zip(before, through(swapped_ref[...]))]
        return tuple(o if carry is None else c + o for c, o in zip(carry or out, out))

    def swap_of(values):
        return [pltpu.roll(v, wide_beams // 2, 1) for v in values]

    if few:
        sums, others = None, []
        for k in range(sets):
            sums = take(k, sums, others if k == sets - 1 else None)
    else:
        zero = jnp.zeros((2 * block, wide_beams), jnp.float32)
        sums = lax.fori_loop(0, sets, take, (zero,) * FRAMES)
        others = swap_of(sums)
    for f in range(FRAMES):
        other = pltpu.roll(others[f], block, 0)
        out = sums[f] + jnp.where(low_row < block, -other, other)
        for p in range(2):
            for s in range(block):
                at = p * block + s
                beam_ref[p, pl.ds(s * FRAMES + f, 1), :] = out[at : at + 1, :beams]

    sent = recv_ref.at[pl.ds(0, count - 1)]
    pltpu.make_async_copy(sent, sent, send_sem).wait()


def class_basis(chan):
    lanes = chan // RADIX
    b = np.arange(lanes)[:, None]
    d = np.arange(lanes)[None, :]
    out = []
    for c in range(RADIX):
        angle = 2.0 * np.pi / chan * (b * (c + RADIX * d) % chan)
        cos, sin = np.cos(angle) * chan**-0.5, np.sin(angle) * chan**-0.5
        out.append(np.block([[cos, -sin], [sin, cos]]))
    return jnp.asarray(np.stack(out), jnp.bfloat16)


def deliver_kernel(power_from, beam_from, power_to, beam_to):
    def deliver(sems):
        copies = [
            pltpu.make_async_copy(power_from, power_to, sems.at[0]),
            pltpu.make_async_copy(beam_from, beam_to, sems.at[1]),
        ]
        for copy in copies:
            copy.start()
        for copy in copies:
            copy.wait()

    pl.run_scoped(deliver, pltpu.SemaphoreType.DMA((2,)))


def on_device(nelem, nchan, voltages, delays, prototype, subband_map, beam_weights):
    parts, elems, samples = voltages.shape
    taps, chan = prototype.shape
    beams, _, block, total = beam_weights.shape
    basis = class_basis(chan)
    count = nelem * nchan
    gather = 8
    wide_beams = max(LANES, 2 * beams)
    out_shape = [
        jax.ShapeDtypeStruct((elems, chan), jnp.bfloat16),
        jax.ShapeDtypeStruct((2, block * FRAMES, beams), jnp.float32),
    ]
    power, beam = pl.pallas_call(
        functools.partial(main_kernel, nelem, nchan, gather),
        in_specs=[pl.BlockSpec(memory_space=pltpu.HBM)] * 6,
        out_specs=[pl.BlockSpec(memory_space=pltpu.VMEM)] * 2,
        out_shape=[pltpu.VMEM(o.shape, o.dtype) for o in out_shape],
        scratch_shapes=[
            pltpu.SMEM(delays.shape, jnp.int32),
            pltpu.SMEM(subband_map.shape, jnp.int32),
            pltpu.VMEM((elems // ROWS, parts, ROWS, samples), jnp.bfloat16),
            pltpu.VMEM((taps, chan), jnp.bfloat16),
            pltpu.VMEM(beam_weights.shape, jnp.bfloat16),
            pltpu.VMEM(basis.shape, jnp.bfloat16),
            pltpu.VMEM((taps, chan), jnp.float32),
            pltpu.VMEM((elems // ROWS, taps, ROWS, chan), jnp.bfloat16),
            pltpu.VMEM((2, 2 * subband_map.shape[0], chan), jnp.bfloat16),
            pltpu.VMEM((parts, FRAMES * elems, chan), jnp.bfloat16),
            pltpu.VMEM((beams * 2 * block, total), jnp.bfloat16),
            pltpu.VMEM((total, block * wide_beams), jnp.bfloat16),
            pltpu.VMEM((gather * elems, block * wide_beams), jnp.bfloat16),
            pltpu.VMEM((nchan, 2 * block, FRAMES * elems), jnp.bfloat16),
            pltpu.VMEM((count, 2 * block, FRAMES * elems), jnp.bfloat16),
            pltpu.SemaphoreType.DMA,
            pltpu.SemaphoreType.DMA((count // gather,)),
        ],
        compiler_params=pltpu.CompilerParams(
            collective_id=0, has_side_effects=True, vmem_limit_bytes=66_400_000
        ),
    )(delays, subband_map, voltages, prototype, beam_weights, basis)
    return pl.pallas_call(
        deliver_kernel,
        in_specs=[pl.BlockSpec(memory_space=pl.ANY)] * 2,
        out_specs=[pl.BlockSpec(memory_space=pl.ANY)] * 2,
        out_shape=out_shape,
        compiler_params=pltpu.CompilerParams(vmem_limit_bytes=2**20),
    )(power, beam)


def solution(mesh):
    return jax.shard_map(
        functools.partial(on_device, mesh.shape["elem"], mesh.shape["chan"]),
        mesh=mesh,
        in_specs=(
            P(None, ("elem", "chan"), None),
            P(("elem", "chan")),
            P(),
            P(),
            P("elem", None, "chan", None),
        ),
        out_specs=(P(("elem", "chan"), None), P(None, "chan", "elem")),
        check_vma=False,
    )
```

```python
import functools
import math

import jax
import jax.numpy as jnp
import numpy as np
from jax import lax
from jax.experimental import pallas as pl
from jax.experimental.pallas import tpu as pltpu
from jax.sharding import PartitionSpec as P

FRAMES = 4
LANES = 128
ROWS = 8
RADIX = 8
LOGICAL = pl.DeviceIdType.LOGICAL
NT = (((1,), (1,)), ((), ()))
TN = (((0,), (0,)), ((), ()))


def cosine(turns, chan):
    y = jnp.abs((turns & (chan - 1)) - chan // 2) - chan // 4
    x = y.astype(jnp.float32) * (2.0 * math.pi / chan)
    s = x * x
    poly = 1.0 / 362880 - s * (1.0 / 39916800)
    poly = -1.0 / 5040 + s * poly
    poly = 1.0 / 120 + s * poly
    poly = -1.0 / 6 + s * poly
    return x + x * s * poly


def sine(turns, chan):
    return cosine(turns + 3 * (chan // 4), chan)


def eight_points(x):
    def add(a, b):
        return (a[0] + b[0], a[1] + b[1])

    def sub(a, b):
        return (a[0] - b[0], a[1] - b[1])

    def minus_i(a):
        return (a[1], -a[0])

    def four(v):
        a, b = add(v[0], v[2]), sub(v[0], v[2])
        c, d = add(v[1], v[3]), minus_i(sub(v[1], v[3]))
        return [add(a, c), add(b, d), sub(a, c), sub(b, d)]

    root = math.sqrt(0.5)
    even = four([add(x[a], x[a + 4]) for a in range(4)])
    d = [sub(x[a], x[a + 4]) for a in range(4)]
    d1 = ((d[1][0] + d[1][1]) * root, (d[1][1] - d[1][0]) * root)
    d3 = ((d[3][1] - d[3][0]) * root, (-d[3][0] - d[3][1]) * root)
    odd = four([d[0], d1, minus_i(d[2]), d3])
    out = []
    for e, o in zip(even, odd):
        out += [e, o]
    return out


def turn_plan(group, delay_ref):
    lane = lax.broadcasted_iota(jnp.int32, (ROWS, LANES), 1)
    sub = lax.broadcasted_iota(jnp.int32, (ROWS, LANES), 0)
    shift = jnp.zeros((ROWS, LANES), jnp.int32)
    for i in range(ROWS):
        shift = jnp.where(sub == i, delay_ref[group * ROWS + i], shift)
    return (lane - shift) & (LANES - 1), lane < LANES - shift, lane < shift


def turn_pair(pair, slot, plan, proto_ref, coef_ref):
    index, stay, _ = plan
    taps, chan = proto_ref.shape
    per = chan // LANES
    for t in range(taps):
        near = [
            jnp.broadcast_to(
                proto_ref[pl.ds(t, 1), pl.ds((2 * pair + i) % per * LANES, LANES)], (ROWS, LANES)
            )
            for i in (-1, 0, 1)
        ]
        turned = [
            jnp.take_along_axis(
                jnp.where(stay, near[i + 1], near[i]), index, axis=1, mode="promise_in_bounds"
            )
            for i in range(2)
        ]
        coef_ref[slot, t, :, pl.ds(2 * pair * LANES, 2 * LANES)] = jnp.concatenate(
            turned, axis=1
        ).astype(jnp.bfloat16)


def filter_pair(group, part, chunk, pair, slot, early, volt_ref, coef_ref, wave_ref):
    _, taps, _, chan = coef_ref.shape
    blocks = FRAMES + taps - 1
    wide = 2 * LANES

    def column(b, size):
        return volt_ref[chunk, part, :, pl.ds(b * chan + pair * wide, size)]

    held = [column(b, wide) for b in range(blocks)]
    if pair == 0:
        last = jnp.concatenate([column(blocks, LANES), held[-1][:, LANES:]], axis=1)
        held = [
            jnp.where(early, nxt, now) for now, nxt in zip(held, [*held[1:], last])
        ]
    stacks = [[] for _ in range(FRAMES)]
    for t in range(taps):
        coef = coef_ref[slot, t, :, pl.ds(pair * wide, wide)]
        for f in range(FRAMES):
            level, term = 0, coef * held[f + t]
            while stacks[f] and stacks[f][-1][0] == level:
                level, term = level + 1, stacks[f].pop()[1] + term
            stacks[f].append((level, term))
    for f in range(FRAMES):
        total = stacks[f].pop()[1]
        while stacks[f]:
            total = stacks[f].pop()[1] + total
        where = pl.ds((group * FRAMES + f) * ROWS, ROWS)
        wave_ref[part, where, pl.ds(pair * wide, wide)] = total


def main_kernel(
    nelem,
    nchan,
    gather,
    delay_hbm,
    map_hbm,
    volt_hbm,
    proto_hbm,
    weight_hbm,
    basis_hbm,
    power_ref,
    beam_ref,
    delay_ref,
    map_ref,
    volt_ref,
    proto_ref,
    raw_ref,
    basis_ref,
    wide_ref,
    coef_ref,
    pick_ref,
    wave_ref,
    weight_ref,
    turned_ref,
    send_ref,
    recv_ref,
    send_sem,
    recv_sem,
):
    parts, wave_rows, chan = wave_ref.shape
    groups = volt_ref.shape[0]
    elems = groups * ROWS
    taps = proto_ref.shape[0]
    per = chan // LANES
    count = nelem * nchan
    elem_at, chan_at = lax.axis_index("elem"), lax.axis_index("chan")
    me = elem_at * nchan + chan_at
    near_start = elem_at < nelem // 2
    barrier = pltpu.get_barrier_semaphore()

    def each_partner(act):
        def row(k, carry):
            first = jnp.where(near_start, nelem - 1 - k, k) * nchan
            for c in range(nchan):

                @pl.when(first + c != me)
                def _():
                    act(first + c, c)

            return carry

        if count <= 64:
            for k in range(nelem):
                row(k, 0)
        else:
            lax.fori_loop(0, nelem, row, 0)

    subbands = map_ref.shape[0]
    block = subbands // nchan
    my_set = me // gather
    beams = raw_ref.shape[0]
    weight_rows, total = weight_ref.shape
    wide_beams = turned_ref.shape[1] // block
    fan = LANES // elems

    def front(local_sem, volt_sem):
        order = [*range(1, groups), 0]
        map_copy = pltpu.make_async_copy(map_hbm, map_ref, local_sem.at[0])
        proto_copy = pltpu.make_async_copy(proto_hbm, proto_ref, local_sem.at[1])
        delay_copy = pltpu.make_async_copy(delay_hbm, delay_ref, local_sem.at[2])
        basis_copy = pltpu.make_async_copy(basis_hbm, basis_ref, local_sem.at[3])
        weight_copy = pltpu.make_async_copy(weight_hbm, raw_ref, local_sem.at[4])
        volt_copies = [
            pltpu.make_async_copy(
                volt_hbm.at[r, pl.ds(order[0] * ROWS, ROWS)], volt_ref.at[0, r], volt_sem.at[r]
            )
            for r in range(parts)
        ]
        for k, g in enumerate(order[1:]):
            volt_copies.append(
                pltpu.make_async_copy(
                    volt_hbm.at[:, pl.ds(g * ROWS, ROWS)],
                    volt_ref.at[k + 1],
                    volt_sem.at[k + parts],
                )
            )
        proto_copy.start()
        delay_copy.start()
        map_copy.start()
        for copy in volt_copies[: parts + 1]:
            copy.start()

        def greet(other, c):
            pl.semaphore_signal(barrier, inc=1, device_id=other, device_id_type=LOGICAL)

        each_partner(greet)
        for copy in volt_copies[parts + 1 :]:
            copy.start()

        map_copy.wait()
        delay_copy.wait()
        proto_copy.wait()
        wide_ref[...] = proto_ref[...].astype(jnp.float32)
        still = jnp.where(me < 0, 1, 0)
        pairs = per // 2
        plans = [turn_plan(g, delay_ref) for g in order]
        turn_pair(0, 0, plans[0], wide_ref, coef_ref)
        def tables():
            row = lax.broadcasted_iota(jnp.int32, (subbands, LANES), 0)
            lane = lax.broadcasted_iota(jnp.int32, (subbands, LANES), 1)
            wanted = jnp.zeros((subbands, LANES), jnp.int32)
            for s in range(subbands):
                wanted = jnp.where(row == s, map_ref[s], wanted)
            scale = chan**-0.5
            cos, sin = cosine(wanted * lane, chan) * scale, sine(wanted * lane, chan) * scale
            cos_step, sin_step = cosine(wanted * LANES, chan), sine(wanted * LANES, chan)
            for j in range(per):
                if j:
                    cos, sin = cos * cos_step - sin * sin_step, sin * cos_step + cos * sin_step
                where = pl.ds(j * LANES, LANES)
                pick_ref[0, pl.ds(0, subbands), where] = cos.astype(jnp.bfloat16)
                pick_ref[0, pl.ds(subbands, subbands), where] = (-sin).astype(jnp.bfloat16)
                pick_ref[1, pl.ds(0, subbands), where] = sin.astype(jnp.bfloat16)
                pick_ref[1, pl.ds(subbands, subbands), where] = cos.astype(jnp.bfloat16)
            column = lax.broadcasted_iota(jnp.int32, (ROWS, LANES), 1)
            column = column // (FRAMES * ROWS) * ROWS + column % ROWS
            late = jnp.zeros((ROWS, LANES), jnp.int32)
            for e in range(elems):
                late = jnp.where(column == e, delay_ref[e], late)
            late = jnp.concatenate([late] * (subbands // ROWS), axis=0)
            cos_late, sin_late = cosine(wanted * late, chan), sine(wanted * late, chan)
            return cos_late, sin_late

        span = FRAMES * ROWS

        def pick(first, size):
            both = sum(
                lax.dot_general(
                    pick_ref[r],
                    wave_ref[r, pl.ds(first, size)],
                    NT,
                    preferred_element_type=jnp.float32,
                )
                for r in range(parts)
            )
            both = [both]
            if first:
                both = [jnp.zeros((2 * subbands, first), jnp.float32), *both]
            if first + size < LANES:
                both.append(jnp.zeros((2 * subbands, LANES - first - size), jnp.float32))
            return jnp.concatenate(both, axis=1)

        units = parts * pairs
        todo = [[] for _ in range(groups * units)]
        for p in range(1, pairs):
            todo[p - 1].append((0, p))
        later = [(n, p) for n in range(1, groups) for p in range(pairs)]
        ahead = [[] for _ in range(groups * units)]
        ahead[pairs - 1], later = later[: pairs - 1], later[pairs - 1 :]
        ahead[2 * pairs - 1], later = later[:1], later[1:]
        ahead[units + parts * pairs - 1] = later
        for n, g in enumerate(order):
            if n < groups - 1:
                volt_copies[n + parts - 1 if n else 0].wait()
            if n == groups - 2:
                basis_copy.start()
                weight_copy.start()
            if n == 1:
                cos_late, sin_late = tables()
            early = plans[n][2].astype(jnp.int32)
            early = jnp.concatenate([early, jnp.zeros_like(early)], axis=1) != 0
            for r in range(parts):
                if n == 0 and r:
                    volt_copies[r].wait()
                if n == groups - 2 and r == parts - 1:
                    volt_copies[-1].wait()
                if n == groups - 2 and r == parts - 1:
                    chosen = pick(span, n * span)
                if n == groups - 1 and r == 0:
                    chosen = chosen + pick(n * span, span)
                for p in range(pairs):
                    for unit, q in ahead[n * units + r * pairs + p]:
                        turn_pair(q, unit + still, plans[unit], wide_ref, coef_ref)
                    filter_pair(g, r, n, p, n, early, volt_ref, coef_ref, wave_ref)
                    for unit, q in todo[n * units + r * pairs + p]:
                        turn_pair(q, unit, plans[unit], wide_ref, coef_ref)
        final = pick(0, span)
        chosen = jnp.where(lax.broadcasted_iota(jnp.int32, final.shape, 1) < span, final, chosen)
        real = chosen[:subbands] * cos_late - chosen[subbands:] * sin_late
        imag = chosen[subbands:] * cos_late + chosen[:subbands] * sin_late
        for c in range(nchan):
            part = slice(c * block, (c + 1) * block)
            send_ref[c] = jnp.concatenate([real[part], imag[part]], axis=0).astype(jnp.bfloat16)

        pl.semaphore_wait(barrier, count - 1)

        def send(other, c):
            pltpu.make_async_remote_copy(
                src_ref=send_ref.at[c],
                dst_ref=recv_ref.at[me],
                send_sem=send_sem,
                recv_sem=recv_sem.at[my_set],
                device_id=other,
                device_id_type=LOGICAL,
            ).start()

        each_partner(send)
        recv_ref[me] = send_ref[chan_at]

        lanes = chan // RADIX
        wave = [wave_ref[r] for r in range(2)]
        split_wave = [
            tuple(wave[r][:, a * lanes : (a + 1) * lanes].astype(jnp.float32) for r in range(2))
            for a in range(RADIX)
        ]
        classes = eight_points(split_wave)
        basis_copy.wait()
        powers = []
        for c in range(RADIX):
            mixed = jnp.concatenate(classes[c], axis=1).astype(jnp.bfloat16)
            spec = jnp.dot(mixed, basis_ref[c], preferred_element_type=jnp.float32)
            both = spec[:, :lanes] * spec[:, :lanes] + spec[:, lanes:] * spec[:, lanes:]
            totals = []
            for g in range(groups):
                tiles = [
                    both[(g * FRAMES + f) * ROWS : (g * FRAMES + f + 1) * ROWS] for f in range(FRAMES)
                ]
                totals.append(sum(tiles[1:], tiles[0]))
            powers.append(jnp.concatenate(totals, axis=0) * (1.0 / FRAMES))
        wide = lanes // RADIX
        at = lax.broadcasted_iota(jnp.int32, (elems, lanes), 1)
        mixed = []
        for e in range(RADIX):
            piece = None
            for c in range(RADIX):
                shift = (wide * (c - e)) % lanes
                moved = pltpu.roll(powers[c], shift, 1) if shift else powers[c]
                piece = moved if piece is None else jnp.where(at // wide == c, moved, piece)
            mixed.append(piece)
        mixed = jnp.concatenate(mixed, axis=0).astype(jnp.bfloat16)
        down = lax.broadcasted_iota(jnp.int32, (lanes, lanes), 0)
        over = lax.broadcasted_iota(jnp.int32, (lanes, lanes), 1)
        back = (over == (down % wide) * RADIX + down // wide).astype(jnp.float32)
        final = jnp.dot(mixed, back.astype(jnp.bfloat16), preferred_element_type=jnp.float32)
        for e in range(RADIX):
            power_ref[:, e * lanes : (e + 1) * lanes] = final[e * elems : (e + 1) * elems].astype(
                jnp.bfloat16
            )

        down = lax.broadcasted_iota(jnp.int32, (weight_rows, block * wide_beams), 0)
        over = lax.broadcasted_iota(jnp.int32, (weight_rows, block * wide_beams), 1)
        target = down % block * wide_beams + down // block % 2 * (wide_beams // 2)
        sort = (over == target + down // (2 * block)).astype(jnp.float32).astype(jnp.bfloat16)
        weight_copy.wait()
        step = min(8, beams)
        for i in range(0, beams, step):
            piece = raw_ref[i : i + step].reshape(step * 2 * block, raw_ref.shape[3])
            weight_ref[2 * block * i : 2 * block * (i + step)] = piece

        def turn_weights(q, carry):
            depth = min(total, 8 * LANES)
            where = pl.multiple_of(q * depth, depth)
            turned = lax.dot_general(
                weight_ref[:, pl.ds(where, depth)], sort, TN, preferred_element_type=jnp.float32
            )
            for z in range(0, depth, LANES):
                tiles = [
                    turned[z + (i * groups + g) * ROWS : z + (i * groups + g + 1) * ROWS]
                    for g in range(groups)
                    for i in range(fan)
                ]
                turned_ref[pl.ds(pl.multiple_of(where + z, LANES), LANES), :] = jnp.concatenate(
                    tiles, axis=0
                ).astype(jnp.bfloat16)
            return carry

        if total <= 8 * LANES:
            turn_weights(0, 0)
        else:
            lax.fori_loop(0, total // (8 * LANES), turn_weights, 0)

    pl.run_scoped(
        front, pltpu.SemaphoreType.DMA((5,)), pltpu.SemaphoreType.DMA((groups + parts - 1,))
    )

    sets = count // gather
    place_at = lax.broadcasted_iota(jnp.int32, (2 * block, LANES), 1) // ROWS % fan
    low_row = lax.broadcasted_iota(jnp.int32, (2 * block, wide_beams), 0)

    def take(k, carry):
        which = jnp.where(near_start, k, sets - 1 - k)
        first = which * gather

        def arrived(n):
            some = recv_ref.at[pl.ds(0, n)]
            pltpu.make_async_copy(some, some, recv_sem.at[which]).wait()

        pl.when(which == my_set)(lambda: arrived(gather - 1))
        pl.when(which != my_set)(lambda: arrived(gather))
        pieces = [[] for _ in range(FRAMES)]
        for q in range(gather // fan):
            tiles = [recv_ref[first + q * fan + i].astype(jnp.float32) for i in range(fan)]
            for f in range(FRAMES):
                piece = None
                for i in range(fan):
                    shift = (ROWS * (i - f)) % LANES
                    moved = pltpu.roll(tiles[i], shift, 1) if shift else tiles[i]
                    piece = moved if piece is None else jnp.where(place_at == i, moved, piece)
                pieces[f].append(piece)
        picked = jnp.concatenate(
            [jnp.concatenate(p, axis=1) for p in pieces], axis=0
        ).astype(jnp.bfloat16)
        depth = gather * elems
        where = pl.multiple_of(which * depth, depth)
        product = jnp.dot(
            picked, turned_ref[pl.ds(where, depth), :], preferred_element_type=jnp.float32
        )
        out = []
        for f in range(FRAMES):
            tile = product[2 * block * f : 2 * block * (f + 1)]
            piece = tile[:, :wide_beams]
            for s in range(1, block):
                piece = jnp.where(
                    low_row % block == s, tile[:, s * wide_beams : (s + 1) * wide_beams], piece
                )
            out.append(piece if carry is None else carry[f] + piece)
        return tuple(out)

    if sets <= 8:
        sums = None
        for k in range(sets):
            sums = take(k, sums)
    else:
        zero = jnp.zeros((2 * block, wide_beams), jnp.float32)
        sums = lax.fori_loop(0, sets, take, (zero,) * FRAMES)
    for f in range(FRAMES):
        other = pltpu.roll(pltpu.roll(sums[f], wide_beams // 2, 1), block, 0)
        out = sums[f] + jnp.where(low_row < block, -other, other)
        for p in range(2):
            for s in range(block):
                at = p * block + s
                beam_ref[p, pl.ds(s * FRAMES + f, 1), :] = out[at : at + 1, :beams]

    sent = recv_ref.at[pl.ds(0, count - 1)]
    pltpu.make_async_copy(sent, sent, send_sem).wait()


def class_basis(chan):
    lanes = chan // RADIX
    b = np.arange(lanes)[:, None]
    d = np.arange(lanes)[None, :]
    out = []
    for c in range(RADIX):
        angle = 2.0 * np.pi / chan * (b * (c + RADIX * d) % chan)
        cos, sin = np.cos(angle) * chan**-0.5, np.sin(angle) * chan**-0.5
        out.append(np.block([[cos, -sin], [sin, cos]]))
    return jnp.asarray(np.stack(out), jnp.bfloat16)


def deliver_kernel(power_from, beam_from, power_to, beam_to):
    def deliver(sems):
        copies = [
            pltpu.make_async_copy(power_from, power_to, sems.at[0]),
            pltpu.make_async_copy(beam_from, beam_to, sems.at[1]),
        ]
        for copy in copies:
            copy.start()
        for copy in copies:
            copy.wait()

    pl.run_scoped(deliver, pltpu.SemaphoreType.DMA((2,)))


def on_device(nelem, nchan, voltages, delays, prototype, subband_map, beam_weights):
    parts, elems, samples = voltages.shape
    taps, chan = prototype.shape
    beams, _, block, total = beam_weights.shape
    basis = class_basis(chan)
    count = nelem * nchan
    gather = 8
    wide_beams = max(LANES, 2 * beams)
    out_shape = [
        jax.ShapeDtypeStruct((elems, chan), jnp.bfloat16),
        jax.ShapeDtypeStruct((2, block * FRAMES, beams), jnp.float32),
    ]
    power, beam = pl.pallas_call(
        functools.partial(main_kernel, nelem, nchan, gather),
        in_specs=[pl.BlockSpec(memory_space=pltpu.HBM)] * 6,
        out_specs=[pl.BlockSpec(memory_space=pltpu.VMEM)] * 2,
        out_shape=[pltpu.VMEM(o.shape, o.dtype) for o in out_shape],
        scratch_shapes=[
            pltpu.SMEM(delays.shape, jnp.int32),
            pltpu.SMEM(subband_map.shape, jnp.int32),
            pltpu.VMEM((elems // ROWS, parts, ROWS, samples), jnp.bfloat16),
            pltpu.VMEM((taps, chan), jnp.bfloat16),
            pltpu.VMEM(beam_weights.shape, jnp.bfloat16),
            pltpu.VMEM(basis.shape, jnp.bfloat16),
            pltpu.VMEM((taps, chan), jnp.float32),
            pltpu.VMEM((elems // ROWS, taps, ROWS, chan), jnp.bfloat16),
            pltpu.VMEM((2, 2 * subband_map.shape[0], chan), jnp.bfloat16),
            pltpu.VMEM((parts, FRAMES * elems, chan), jnp.bfloat16),
            pltpu.VMEM((beams * 2 * block, total), jnp.bfloat16),
            pltpu.VMEM((total, block * wide_beams), jnp.bfloat16),
            pltpu.VMEM((nchan, 2 * block, FRAMES * elems), jnp.bfloat16),
            pltpu.VMEM((count, 2 * block, FRAMES * elems), jnp.bfloat16),
            pltpu.SemaphoreType.DMA,
            pltpu.SemaphoreType.DMA((count // gather,)),
        ],
        compiler_params=pltpu.CompilerParams(
            collective_id=0, has_side_effects=True, vmem_limit_bytes=66_400_000
        ),
    )(delays, subband_map, voltages, prototype, beam_weights, basis)
    return pl.pallas_call(
        deliver_kernel,
        in_specs=[pl.BlockSpec(memory_space=pl.ANY)] * 2,
        out_specs=[pl.BlockSpec(memory_space=pl.ANY)] * 2,
        out_shape=out_shape,
        compiler_params=pltpu.CompilerParams(vmem_limit_bytes=2**20),
    )(power, beam)


def solution(mesh):
    return jax.shard_map(
        functools.partial(on_device, mesh.shape["elem"], mesh.shape["chan"]),
        mesh=mesh,
        in_specs=(
            P(None, ("elem", "chan"), None),
            P(("elem", "chan")),
            P(),
            P(),
            P("elem", None, "chan", None),
        ),
        out_specs=(P(("elem", "chan"), None), P(None, "chan", "elem")),
        check_vma=False,
    )
```
